32 devices in a mesh: cell: 8 (over z, y), spot: 4 (over x, core).
Axes of the slice: x: 2, y: 2, z: 4, core: 2. Of those that a mesh axis runs over, the one named last changes fastest.
Arguments:
- logits: float32 [2, 22528, 2048], P(None, 'cell', 'spot'), may hold values from -9 to 12.5
- filter_logits: float32 [2, 22528], P(None, 'cell'), may hold values from -6 to 9
- expression: float32 [22528, 2048], P('cell', 'spot'), may hold values from 0.1 to 10
- observed: float32 [2, 2048, 2048], P(None, 'cell', 'spot'), may hold values from 0.1 to 30
- gene_mask: int32 [4, 2048], P(None, 'cell'), may hold values 0 or 1
- slide_ids: int32 [2048], P('spot'), may hold values from 0 to 3
- true_counts: int32 [4], replicated, may hold values from 128 to 511
Outputs:
- grad_logits: float32 [2, 22528, 2048], P(None, 'cell', 'spot')
- grad_filter: float32 [2, 22528], P(None, 'cell')
- count_terms: float32 [2, 4], replicated
- loss: float32 [], replicated
The draws below stay inside these ranges and needn't reach their ends.
All inputs are finite; a program needn't handle non-finite values. No bound on the sum of `gene_mask` on one device may be relied on, other than what follows from the above.
Results may differ from the reference program's by a relative error of at most 0.0003.
Values sent between devices are 32-bit elements; how exact they have to be, the bound alone decides.
No kernel may reach another device: no remote copies, remote signals or barrier semaphores. Data moves between devices by JAX's collectives and lax.ppermute only.
A program may use at most 128 MiB of HBM per device.

```python
import math
import jax
import jax.numpy as jnp
from jax import lax

G = 2048
SLIDES = 4
LAYERS = 2
CELLS = 22528
SPOTS = 2048


def draw_logits(key, part):
    first, second = jax.random.split(key)
    noise = 1.5 * jnp.clip(jax.random.normal(first, (LAYERS, CELLS, SPOTS), jnp.float32), -6.0, 6.0)
    shift = jax.random.uniform(second, (LAYERS, CELLS, 1), jnp.float32, 0.0, 2.3)
    ramp = 1.0986 * jnp.arange(CELLS, dtype=jnp.float32) / CELLS
    return noise + shift + ramp[None, :, None]


def draw_filter_logits(key, part):
    noise = 1.2 * jnp.clip(jax.random.normal(key, (LAYERS, CELLS), jnp.float32), -5.0, 5.0)
    ramp = 3.0 * jnp.arange(CELLS, dtype=jnp.float32) / CELLS
    return noise + ramp[None, :]


def draw_observed(key, part):
    first = jax.random.fold_in(key, 0)
    base = jnp.exp(jax.random.uniform(first, (LAYERS, G, SPOTS), jnp.float32, -2.3, 2.3))
    ramp = 1.0 + 2.0 * jnp.arange(SPOTS, dtype=jnp.float32) / SPOTS
    return base * ramp[None, None, :]


def place_ends(drawn, key, smallest, largest):
    spot = [jax.random.randint(jax.random.fold_in(key, axis), (), 0, length) for axis, length in enumerate(drawn.shape)]
    widest = drawn.shape.index(max(drawn.shape))
    beside = spot[:widest] + [(spot[widest] + 1) % drawn.shape[widest]] + spot[widest + 1:]
    return drawn.at[tuple(spot)].set(smallest).at[tuple(beside)].set(largest)


def levels(stream_key, shape, pieces, least, high):
    level, own = 1.0, jax.random.fold_in(stream_key, 6)
    for axis_at, parts in pieces:
        steps = jnp.exp(jax.random.uniform(jax.random.fold_in(own, axis_at), (parts,), jnp.float32, least / len(pieces), high / len(pieces)))
        level = level * jnp.repeat(steps, shape[axis_at] // parts).reshape([-1 if axis == axis_at else 1 for axis in range(len(shape))])
    return level


def setup_inputs(seed: int = 0) -> dict:
    arg_keys = jax.random.split(jax.random.key(seed), 8)
    logits = draw_logits(jax.random.fold_in(arg_keys[7], 71), 0)
    filter_logits = draw_filter_logits(jax.random.fold_in(arg_keys[7], 71), 0)
    expression = jnp.clip(jnp.exp(math.log(10.0) - 4.6051702 * jax.random.uniform(arg_keys[2], (CELLS, G), jnp.float32) ** levels(arg_keys[2], (CELLS, G), ((0, 8), (1, 4)), -0.2, 0.2)), 0.1, 10.0)
    observed = draw_observed(jax.random.fold_in(arg_keys[7], 71), 0)
    gene_mask = place_ends((jax.random.randint(arg_keys[4], (SLIDES, G), 0, 2) < 1).astype(jnp.int32), jax.random.fold_in(arg_keys[4], 1), 0, 1)
    slide_ids = place_ends(jax.random.randint(arg_keys[5], (SPOTS,), 0, SLIDES), jax.random.fold_in(arg_keys[5], 1), 0, SLIDES - 1).astype(jnp.int32)
    true_counts = place_ends(jax.random.randint(arg_keys[6], (SLIDES,), SPOTS // (4 * SLIDES), SPOTS // SLIDES), jax.random.fold_in(arg_keys[6], 1), SPOTS // (4 * SLIDES), (SPOTS // SLIDES) - 1).astype(jnp.int32)
    return dict(logits=logits, filter_logits=filter_logits, expression=expression, observed=observed, gene_mask=gene_mask, slide_ids=slide_ids, true_counts=true_counts)


count_weight = 0.0625
entropy_weight = 1.0
epsilon = 1e-06
HIGH = lax.Precision.HIGHEST

@jax.custom_vjp
def low(v):
    return lax.optimization_barrier(v.astype(jnp.bfloat16)).astype(jnp.float32)

@jax.custom_vjp
def low_back(v):
    return v

def low_keep(v):
    return (low(v), None)

def low_pass(kept, grad):
    return (grad,)

def back_keep(v):
    return (v, None)

def back_low(kept, grad):
    return (low(grad),)
low.defvjp(low_keep, low_pass)
low_back.defvjp(back_keep, back_low)

def layer_loss(scores, gates, expression, observed, weight_mask, onehot, counts):
    column_top = lax.optimization_barrier(jnp.max(scores, axis=0))
    exponent = jnp.exp(scores - column_top[None, :])
    mapping = exponent / lax.optimization_barrier(jnp.sum(exponent, axis=0))[None, :]
    kept = jax.nn.sigmoid(gates)
    weighted = kept[:, None] * mapping
    column_mass = lax.optimization_barrier(jnp.sum(weighted, axis=0))
    projected = lax.dot_general(expression, weighted, (((0,), (0,)), ((), ())), precision=HIGH, preferred_element_type=jnp.float32)
    cross = jnp.dot(projected * observed, onehot, precision=HIGH)
    power = jnp.dot(projected * projected, onehot, precision=HIGH)
    own = jnp.dot(observed * observed, onehot, precision=HIGH)
    cosine = cross * lax.rsqrt(power + epsilon) * lax.rsqrt(own + epsilon)
    gene_term = -jnp.sum(weight_mask * cosine) / G
    slide_mass = jnp.dot(column_mass, onehot, precision=HIGH)
    terms = count_weight * ((slide_mass - counts) / counts) ** 2
    entropy = jnp.mean(kept * jax.nn.softplus(-gates) + (1.0 - kept) * jax.nn.softplus(gates))
    return (gene_term + jnp.sum(terms) + entropy_weight * entropy, terms)

def reference(logits, filter_logits, expression, observed, gene_mask, slide_ids, true_counts):
    onehot = (slide_ids[:, None] == jnp.arange(SLIDES, dtype=jnp.int32)[None, :]).astype(jnp.float32)
    weight_mask = gene_mask.T.astype(jnp.float32)
    counts = true_counts.astype(jnp.float32)

    def forward(scores, gates):
        total = jnp.zeros((), jnp.float32)
        terms_all = []
        for layer in range(LAYERS):
            value, terms = layer_loss(scores[layer], gates[layer], expression, observed[layer], weight_mask, onehot, counts)
            total = total + value
            terms_all.append(terms)
        return (total, jnp.stack(terms_all))
    loss, vjp_fn, count_terms = jax.vjp(forward, logits, filter_logits, has_aux=True)
    grad_scores, grad_gates = vjp_fn(jnp.ones((), jnp.float32))
    return (grad_scores * (CELLS * G), grad_gates * CELLS, count_terms, loss)
```

```python
import functools
import math

import jax
import jax.numpy as jnp
from jax import lax
from jax.experimental import pallas as pl
from jax.experimental.pallas import tpu as pltpu
from jax.sharding import PartitionSpec as P

G = 2048
SLIDES = 4
COUNT_WEIGHT = 0.0625
ENTROPY_WEIGHT = 1.0
EPSILON = 1e-06
HIGHEST = lax.Precision.HIGHEST
SETS = [256, 256]
EARLY = [False]
F32 = jnp.float32
BF16 = jnp.bfloat16
NN = (((1,), (0,)), ((), ()))
NT = (((1,), (1,)), ((), ()))
TN = (((0,), (0,)), ((), ()))


def ring_order(n):
    if n < 8:
        return list(range(n))
    ys = math.isqrt(n // 2)
    zs = n // ys
    walk = [(z, 0) for z in range(zs)]
    for i, z in enumerate(reversed(range(zs))):
        cols = range(1, ys)
        walk += [(z, y) for y in (cols if i % 2 == 0 else reversed(cols))]
    return [z * ys + y for z, y in walk]


def split(v):
    hi = v.astype(BF16)
    return hi, (v - hi.astype(F32)).astype(BF16)


def mm(a, b, dims=NN):
    return lax.dot_general(a, b, dims, preferred_element_type=F32)


def mm_onehot(onehot, v, dims):
    hi, lo = split(v)
    if dims is TN:
        return mm(hi, onehot, dims) + mm(lo, onehot, dims)
    return mm(onehot, hi, dims) + mm(onehot, lo, dims)


def mm_exact(a, b, dims=NN):
    return lax.dot_general(a, b, dims, precision=HIGHEST, preferred_element_type=F32)


def row_tile(rows):
    return rows // 2 if rows % 256 == 0 else rows


def tie(v, *others):
    return lax.optimization_barrier((v, *others))[0]


def prep_kernel(x_ref, kept_ref, hi_ref, lo_ref, sum_ref):
    i = pl.program_id(1)
    e = jnp.exp(x_ref[0])
    rows, cols = e.shape
    kept = jnp.transpose(jnp.broadcast_to(kept_ref[0], (128, rows)))
    u = e * jnp.tile(kept, (1, cols // 128))

    @pl.when(i == 0)
    def _():
        sum_ref[...] = jnp.zeros_like(sum_ref)

    sum_ref[0, 0:1, :] += jnp.sum(e, axis=0, keepdims=True)
    sum_ref[0, 1:2, :] += jnp.sum(u, axis=0, keepdims=True)
    hi, lo = split(jnp.transpose(u))
    hi_ref[...] = hi
    lo_ref[...] = lo


def prep(x, kept):
    layers, rows, cols = x.shape
    tile = row_tile(rows)
    wide = pl.BlockSpec((cols, tile), lambda l, i: (l, i))
    return pl.pallas_call(
        prep_kernel,
        grid=(layers, rows // tile),
        in_specs=[
            pl.BlockSpec((1, tile, cols), lambda l, i: (l, i, 0)),
            pl.BlockSpec((1, 1, tile), lambda l, i: (l, 0, i)),
        ],
        out_specs=[wide, wide, pl.BlockSpec((1, 8, cols), lambda l, i: (l, 0, 0))],
        out_shape=[
            jax.ShapeDtypeStruct((layers * cols, rows), BF16),
            jax.ShapeDtypeStruct((layers * cols, rows), BF16),
            jax.ShapeDtypeStruct((layers, 8, cols), F32),
        ],
        name="prep",
        cost_estimate=pl.CostEstimate(
            flops=10 * layers * rows * cols,
            bytes_accessed=8 * layers * rows * cols,
            transcendentals=layers * rows * cols,
        ),
    )(x, kept.reshape(layers, 1, rows))


def fwd_kernel(n, unit, cols, has_sums, me_ref, hi_hbm, lo_hbm, *refs):
    exprs, refs = refs[: len(cols)], refs[len(cols) :]
    sums_ref, refs = (refs[0], refs[1:]) if has_sums else (None, refs)
    outs, (hi, lo, expr, acc, turn, sems) = refs[:n], refs[n:]
    steps, chunk, genes = expr.shape

    def copies(i):
        at = pl.ds(pl.multiple_of(i * chunk, chunk), chunk)
        todo = [
            pltpu.make_async_copy(hi_hbm.at[:, at], hi.at[i], sems.at[0, i]),
            pltpu.make_async_copy(lo_hbm.at[:, at], lo.at[i], sems.at[1, i]),
        ]
        to = 0
        for j, (e, (col, w)) in enumerate(zip(exprs, cols)):
            todo.append(
                pltpu.make_async_copy(
                    e.at[at, col : col + w], expr.at[i, :, to : to + w], sems.at[2 + j, i]
                )
            )
            to += w
        return todo

    def start(i, carry):
        for c in copies(i):
            c.start()
        return carry

    def multiply(i, carry):
        for c in copies(i):
            c.wait()
        eh, el = split(expr[i])
        part = mm(hi[i], eh) + mm(lo[i], eh) + mm(hi[i], el)
        acc[...] = jnp.where(i == 0, part, acc[...] + part)
        return carry

    lax.fori_loop(0, steps, start, 0)
    lax.fori_loop(0, steps, multiply, 0)
    own = unit // n
    row = 0
    for at in range(0, genes, unit):
        turn[...] = jnp.transpose(acc[:, at : at + unit])
        for d in range(n):
            p = lax.rem(me_ref[0] + d, n)
            outs[d][row : row + own, :] = turn[pl.ds(pl.multiple_of(p * own, own), own), :]
        row += own
    if has_sums:
        layers, _, lanes = sums_ref.shape
        for d in range(n):
            for l in range(layers):
                outs[d][row : row + 8, l * lanes : (l + 1) * lanes] = sums_ref[l]


def forward(n, unit, me, hi, lo, exprs, sums=None):
    wide, rows = hi.shape
    chunk = 256 if rows % 256 == 0 else rows
    steps = rows // chunk
    genes = sum(w for _, _, w in exprs)
    out_rows = genes // n + (8 if sums is not None else 0)
    anywhere = pl.BlockSpec(memory_space=pl.ANY)
    in_specs = [pl.BlockSpec(memory_space=pltpu.SMEM)] + [anywhere] * (2 + len(exprs))
    args = [me, hi, lo] + [e for e, _, _ in exprs]
    if sums is not None:
        in_specs.append(pl.BlockSpec(memory_space=pltpu.VMEM))
        args.append(sums)
    cols = [(c, w) for _, c, w in exprs]
    return pl.pallas_call(
        functools.partial(fwd_kernel, n, unit, cols, sums is not None),
        in_specs=in_specs,
        out_shape=[jax.ShapeDtypeStruct((out_rows, wide), F32)] * n,
        scratch_shapes=[
            pltpu.VMEM((steps, wide, chunk), BF16),
            pltpu.VMEM((steps, wide, chunk), BF16),
            pltpu.VMEM((steps, chunk, genes), F32),
            pltpu.VMEM((wide, genes), F32),
            pltpu.VMEM((unit, wide), F32),
            pltpu.SemaphoreType.DMA((2 + len(exprs), steps)),
        ],
        name="fwd",
        cost_estimate=pl.CostEstimate(
            flops=6 * wide * rows * genes,
            bytes_accessed=4 * wide * rows + 4 * rows * genes + 4 * wide * genes,
            transcendentals=0,
        ),
    )(*args)


def deal_kernel(place, unit, obs_ref, mask_ref, out_ref):
    n = len(place)
    layers, rows, _ = obs_ref.shape
    own, units = unit // n, rows // unit
    cut = layers * units * own
    out_ref[:, cut:, :] = jnp.zeros((n, out_ref.shape[1] - cut, out_ref.shape[2]), F32)
    for j in range(n):
        for u in range(units):
            src = slice(u * unit + place[j] * own, u * unit + (place[j] + 1) * own)
            for l in range(layers):
                to = (l * units + u) * own
                out_ref[j, to : to + own, :] = obs_ref[l, src, :]
            slides = mask_ref.shape[0]
            out_ref[j, cut + 8 * u : cut + 8 * u + slides, 0:own] = mask_ref[:, src].astype(F32)


def deal(ring, unit, me, observed, gene_mask):
    layers, rows, cols = observed.shape
    n, own = ring.n, unit // ring.n
    if rows % unit:
        observed = lax.all_gather(observed, "cell", axis=1, tiled=True)
        gene_mask = lax.all_gather(gene_mask, "cell", axis=1, tiled=True)
        units = observed.shape[1] // unit
        pick = lambda a, at: lax.dynamic_index_in_dim(a, me[0], at, keepdims=False)
        obs = pick(observed.reshape(layers, units, n, own, cols), 2)
        mask = pick(gene_mask.astype(F32).reshape(-1, units, n, own), 2).transpose(1, 0, 2)
        mask = jnp.pad(mask, ((0, 0), (0, 8 - mask.shape[1]), (0, cols - own)))
        slab = jnp.concatenate([obs.reshape(-1, cols), mask.reshape(-1, cols)])
        return slab[None], units
    units = rows // unit
    out = pl.pallas_call(
        functools.partial(deal_kernel, ring.place, unit),
        out_shape=jax.ShapeDtypeStruct((n, layers * units * own + 8 * units, cols), F32),
        name="deal",
    )(observed, gene_mask)
    return lax.all_to_all(out, "cell", 0, 0, tiled=True), units


def slide_rows(ids_ref, cols):
    return lax.broadcasted_iota(jnp.int32, (8, cols), 0) == ids_ref[...]


def held_rows(qs, at, lane, inv):
    return jnp.concatenate([q[r : r + rows, lane] for q, (r, rows) in zip(qs, at)], 0) * inv[:, lane]


class Dealt:
    def __init__(self, units, block_units, first, count, own, layers, blocks):
        self.units, self.block_units = units, block_units
        self.first, self.count, self.own = first, count, own
        self.layers, self.blocks = layers, blocks

    def places(self, me_ref):
        for j in range(self.blocks):
            for u in range(self.first, self.first + self.count):
                unit = me_ref[1 + j] * self.block_units + u
                yield unit // self.units, unit % self.units

    def obs(self, me_ref, slab_ref, l):
        rows = [
            slab_ref[s, pl.ds(pl.multiple_of((l * self.units + u) * self.own, self.own), self.own), :]
            for s, u in self.places(me_ref)
        ]
        return jnp.concatenate(rows, 0)

    def mask(self, me_ref, slab_ref):
        cut = self.layers * self.units * self.own
        cols = [
            slab_ref[s, pl.ds(pl.multiple_of(cut + 8 * u, 8), 8), 0 : self.own]
            for s, u in self.places(me_ref)
        ]
        return jnp.concatenate(cols, 1)


def stats_kernel(dealt, at, first, me_ref, ids_ref, tot_ref, slab_ref, *refs):
    qs, out_ref = refs[:-1], refs[-1]
    cols = ids_ref.shape[1]
    layers = tot_ref.shape[1] // cols
    onehot = slide_rows(ids_ref, cols).astype(F32)
    marks = onehot.astype(BF16)
    inv = 1.0 / tot_ref[-8:-7, :]
    for l in range(layers):
        lane = slice(l * cols, (l + 1) * cols)
        proj = held_rows(qs, at, lane, inv)
        obs = dealt.obs(me_ref, slab_ref, l)
        out_ref[24 * l : 24 * l + 8, :] = mm_onehot(marks, proj * obs, NT)
        out_ref[24 * l + 8 : 24 * l + 16, :] = mm_onehot(marks, proj * proj, NT)
        out_ref[24 * l + 16 : 24 * l + 24, :] = mm_onehot(marks, obs * obs, NT)
        if first:
            mass = onehot * (tot_ref[-7:-6, lane] * inv[:, lane])
            row = 24 * layers + 8 * l
            out_ref[row : row + 8, :] = jnp.broadcast_to(
                jnp.sum(mass, axis=1, keepdims=True), (8, out_ref.shape[1])
            )


SMEM_VMEM = lambda smem, vmem: [pl.BlockSpec(memory_space=pltpu.SMEM)] * smem + [
    pl.BlockSpec(memory_space=pltpu.VMEM)
] * vmem


def stats(dealt, me, ids, totals, slab, qs, at, first):
    layers = totals.shape[1] // ids.shape[1]
    genes = sum(r for _, r in at)
    return pl.pallas_call(
        functools.partial(stats_kernel, dealt, at, first),
        in_specs=SMEM_VMEM(1, 3 + len(qs)),
        out_shape=jax.ShapeDtypeStruct(((32 if first else 24) * layers, genes), F32),
        name="stats",
    )(me, ids, totals, slab, *qs)


def swap_lanes(v, group, shift):
    count, size = group
    run = count * size
    out = []
    for base in range(0, v.shape[1], run):
        for i in range(count):
            j = (i - shift) % count
            out.append(v[:, base + j * size : base + (j + 1) * size])
    return jnp.concatenate(out, 1)


def grad_kernel(shifts, dealt, at, xs, first, me_ref, ent_ref, *refs):
    ids_ref, tot_ref, slab_ref, extra_ref = refs[:4]
    refs = refs[4:]
    st_refs, refs = refs[: len(shifts)], refs[len(shifts) :]
    qs, (out_ref, aux_ref) = refs[:-2], refs[-2:]
    cols = ids_ref.shape[1]
    layers = tot_ref.shape[1] // cols
    genes = st_refs[0].shape[1]
    own = genes // (2 * xs)
    onehot = slide_rows(ids_ref, cols).astype(F32)
    marks = onehot.astype(BF16)
    inv = 1.0 / tot_ref[-8:-7, :]
    st = None
    for (dx, dc), ref in zip(shifts, st_refs):
        v = ref[...]
        if dc:
            v = swap_lanes(v, (2, own), 1)
        if dx:
            v = swap_lanes(v, (xs, 2 * own), dx)
        st = v if st is None else st + v
    mask = dealt.mask(me_ref, slab_ref)
    aux_ref[...] = jnp.zeros_like(aux_ref)
    out_rows = out_ref.shape[0]
    if out_rows > genes:
        out_ref[genes:out_rows, :] = jnp.full((out_rows - genes, layers * cols), ent_ref[0], F32)
    for l in range(layers):
        lane = slice(l * cols, (l + 1) * cols)
        cross = st[24 * l : 24 * l + 8]
        inv_proj = lax.rsqrt(st[24 * l + 8 : 24 * l + 16] + EPSILON)
        inv_obs = lax.rsqrt(st[24 * l + 16 : 24 * l + 24] + EPSILON)
        weight = mask * (-1.0 / G)
        term = jnp.sum(weight * (cross * inv_proj * inv_obs), axis=0, keepdims=True)
        spread_first = mm_onehot(marks, weight * inv_proj * inv_obs, TN)
        spread_second = mm_onehot(
            marks, weight * cross * (inv_proj * inv_proj * inv_proj) * inv_obs, TN
        )
        proj = held_rows(qs, at, lane, inv)
        grad = spread_first * dealt.obs(me_ref, slab_ref, l) - spread_second * proj
        out_ref[0:genes, lane] = grad
        back = jnp.sum(grad * proj, axis=0, keepdims=True)
        term = jnp.concatenate([term, jnp.zeros((1, cols - genes), F32)], 1)
        if first:
            mass = st[24 * layers + 8 * l : 24 * layers + 8 * l + 8]
            counts = extra_ref[:, :genes]
            off = (mass - counts) / counts
            slope = 2.0 * COUNT_WEIGHT * (mass - counts) / (counts * counts)
            aux_ref[1:2, lane] = jnp.sum(onehot * slope[:, 0:1], axis=0, keepdims=True)
            aux_ref[8:16, l * cols : l * cols + genes] = COUNT_WEIGHT * (off * off)
        else:
            back = back + extra_ref[0:1, lane]
            term = term + extra_ref[2:3, lane]
        aux_ref[0:1, lane] = back
        aux_ref[2:3, lane] = term
        if out_rows > genes:
            out_ref[genes : genes + 1, lane] = back
            out_ref[genes + 1 : genes + 2, lane] = term


def grads(shifts, dealt, xs, me, ent, ids, totals, slab, extra, sts, qs, at, first, last):
    genes, wide = sum(r for _, r in at), totals.shape[1]
    return pl.pallas_call(
        functools.partial(grad_kernel, shifts, dealt, at, xs, first),
        in_specs=SMEM_VMEM(2, 4 + len(sts) + len(qs)),
        out_shape=[
            jax.ShapeDtypeStruct((genes + (8 if last else 0), wide), F32),
            jax.ShapeDtypeStruct((16, wide), F32),
        ],
        name="grads",
    )(me, ent, ids, totals, slab, extra, *sts, *qs)


def gather_rows(n, unit, me_ref, offsets, blocks, hi, lo):
    own = unit // n
    for d, block in zip(offsets, blocks):
        p = lax.rem(me_ref[0] + d + n, n)
        for j in range(hi.shape[0] // unit):
            h, lw = split(block[j * own : (j + 1) * own, :])
            at = pl.ds(pl.multiple_of(j * unit + p * own, own), own)
            hi[at, :] = h
            lo[at, :] = lw


def product(exprs, hi, lo, lanes):
    eh, el = split(jnp.concatenate([e[...] for e in exprs], 1))
    gh, gl = hi[:, lanes], lo[:, lanes]
    return mm(eh, gh) + mm(eh, gl) + mm(el, gh)


def bwd_first_kernel(n, unit, offsets, priors, me_ref, *refs):
    out_ref, hi, lo = refs[-3:]
    prior, refs = refs[:priors], refs[priors:]
    blocks = refs[: len(offsets)]
    exprs = refs[len(offsets) : -3]

    @pl.when(pl.program_id(0) == 0)
    def _():
        gather_rows(n, unit, me_ref, offsets, blocks, hi, lo)

    total = product(exprs, hi, lo, slice(None))
    for p in prior:
        total = total + p[...]
    out_ref[...] = total


def bwd_last_kernel(n, unit, offsets, scale, splits, me_ref, *refs):
    x_ref, kept_ref, tot_ref, aux_ref = refs[:4]
    refs = refs[4:]
    priors, refs = refs[: len(splits)], refs[len(splits) :]
    grad_ref, filt_ref, hi, lo, back = refs[-5:]
    blocks = refs[: len(offsets)]
    exprs = refs[len(offsets) : -5]
    layers, rows, cols = x_ref.shape

    @pl.when(pl.program_id(0) == 0)
    def _():
        gather_rows(n, unit, me_ref, offsets, blocks, hi, lo)
        total = blocks[0][-8:, :]
        for b in blocks[1:]:
            total += b[-8:, :]
        back[...] = total
        for l in range(layers):
            lane = slice(l * cols, (l + 1) * cols)
            inv = 1.0 / tot_ref[-8:-7, lane]
            mass = tot_ref[-7:-6, lane] * inv
            back[2:3, lane] = inv
            back[3:4, lane] = total[0:1, lane] + aux_ref[1:2, lane] * mass

    ones = jnp.ones((8, cols), F32)
    for l in range(layers):
        lane = slice(l * cols, (l + 1) * cols)
        gw = product(exprs, hi, lo, lane)
        if splits:
            held = [p[:, lane] for p in priors]
            gw = gw + functools.reduce(
                lambda low, j: jnp.where(pl.program_id(0) < splits[j], low, held[j]),
                range(1, len(held)),
                held[0],
            )
        gw = gw + aux_ref[1:2, lane]
        mapping = jnp.exp(x_ref[l]) * back[2:3, lane]
        kept = jnp.transpose(jnp.broadcast_to(kept_ref[l], (128, rows)))
        kept = jnp.tile(kept, (1, cols // 128))
        grad_ref[l] = scale * (mapping * (kept * gw - back[3:4, lane]))
        filt_ref[l] = mm_exact(ones, mapping * gw, NT)[0:1, :]


def backward_first(n, unit, offsets, me, prior, blocks, exprs, begin, rows):
    tile = rows // 4 if rows % 32 == 0 else rows
    wide = blocks[0].shape[1]
    genes = sum(w for _, _, w in exprs)
    skip = begin // tile
    whole = pl.BlockSpec(blocks[0].shape, lambda i: (0, 0))
    return pl.pallas_call(
        functools.partial(bwd_first_kernel, n, unit, offsets, len(prior)),
        grid=(rows // tile,),
        in_specs=[pl.BlockSpec(memory_space=pltpu.SMEM)]
        + [pl.BlockSpec((tile, wide), lambda i: (i, 0))] * len(prior)
        + [whole] * len(blocks)
        + [pl.BlockSpec((tile, w), lambda i, c=c: (i + skip, c)) for _, c, w in exprs],
        out_specs=pl.BlockSpec((tile, wide), lambda i: (i, 0)),
        out_shape=jax.ShapeDtypeStruct((rows, wide), F32),
        scratch_shapes=[pltpu.VMEM((genes, wide), BF16), pltpu.VMEM((genes, wide), BF16)],
        name="bwd_first",
        cost_estimate=pl.CostEstimate(
            flops=6 * rows * genes * wide,
            bytes_accessed=4 * rows * (genes + wide) + 4 * genes * wide,
            transcendentals=0,
        ),
    )(me, *prior, *blocks, *[e for e, _, _ in exprs])


def backward_last(n, unit, offsets, scale, me, x, kept, totals, aux, prior, blocks, exprs):
    tile = 256
    layers, rows, cols = x.shape
    wide = layers * cols
    genes = sum(w for _, _, w in exprs)
    fixed = lambda a: pl.BlockSpec(a.shape, lambda i: (0,) * a.ndim)
    args = [me, x, kept.reshape(layers, 1, rows), totals, aux]
    in_specs = [
        pl.BlockSpec(memory_space=pltpu.SMEM),
        pl.BlockSpec((layers, tile, cols), lambda i: (0, i, 0)),
        pl.BlockSpec((layers, 1, tile), lambda i: (0, 0, i)),
        fixed(totals),
        fixed(aux),
    ]
    args += prior
    splits = []
    for p in prior:
        begin = splits[-1] + prior[len(splits) - 1].shape[0] // tile if splits else 0
        splits.append(begin)
        steps = p.shape[0] // tile
        in_specs.append(
            pl.BlockSpec(
                (tile, wide), lambda i, b=begin, t=steps: (jnp.clip(i - b, 0, t - 1), 0)
            )
        )
    args += list(blocks) + [e for e, _, _ in exprs]
    in_specs += [fixed(b) for b in blocks]
    in_specs += [pl.BlockSpec((tile, w), lambda i, c=c: (i, c)) for _, c, w in exprs]
    return pl.pallas_call(
        functools.partial(bwd_last_kernel, n, unit, offsets, scale, splits),
        grid=(rows // tile,),
        in_specs=in_specs,
        out_specs=[
            pl.BlockSpec((layers, tile, cols), lambda i: (0, i, 0)),
            pl.BlockSpec((layers, 1, tile), lambda i: (0, 0, i)),
        ],
        out_shape=[
            jax.ShapeDtypeStruct((layers, rows, cols), F32),
            jax.ShapeDtypeStruct((layers, 1, rows), F32),
        ],
        scratch_shapes=[
            pltpu.VMEM((genes, wide), BF16),
            pltpu.VMEM((genes, wide), BF16),
            pltpu.VMEM((8, wide), F32),
        ],
        name="bwd_last",
        cost_estimate=pl.CostEstimate(
            flops=6 * rows * genes * wide,
            bytes_accessed=4 * rows * (genes + 3 * wide) + 4 * genes * wide,
            transcendentals=rows * wide,
        ),
    )(*args)


class Ring:
    def __init__(self, n):
        self.n = n
        order = ring_order(n)
        self.place = [order.index(i) for i in range(n)]
        right = [(order[i], order[(i + 1) % n]) for i in range(n)]
        self.dirs = (right, [(b, a) for a, b in right])
        self.far = n // 2
        self.near = n - 1 - self.far

    def hop(self, v, way):
        return lax.ppermute(v, "cell", self.dirs[way])


class Scatter:
    def __init__(self, ring, v, flip):
        self.ring, self.v, self.flip = ring, v, flip
        self.sign = -1 if flip else 1
        self.step = 0
        self.flying = False
        self.r, self.l = self.at(ring.far), self.at(-ring.near)

    def at(self, d):
        return self.v[(self.sign * d) % self.ring.n]

    def hop(self):
        ring = self.ring
        self.mark = self.r
        self.r = ring.hop(self.r, int(self.flip))
        if self.step < ring.near:
            self.l = ring.hop(self.l, 1 - int(self.flip))
        self.step += 1
        self.flying = True

    def add(self, *after):
        ring, s = self.ring, self.step - 1
        self.flying = False
        if after:
            self.r, self.l = lax.optimization_barrier((self.r, self.l, *after))[:2]
        if s < ring.far - 1:
            self.r = self.r + self.at(ring.far - 1 - s)
        if s < ring.near - 1:
            self.l = self.l + self.at(s + 1 - ring.near)
        if self.step == ring.far:
            self.r = self.r + self.l + self.at(0)

    def advance(self, *after):
        if self.flying:
            self.add(*after)
        if self.step < self.ring.far:
            self.hop()

    def finish(self):
        while self.flying:
            self.advance()
        return self.r


class Gather:
    def __init__(self, ring, v, flip):
        self.ring, self.flip = ring, flip
        self.sign = -1 if flip else 1
        self.blocks, self.offsets = [v], [0]
        self.r = self.l = v
        self.step = 0

    def advance(self, *after):
        ring = self.ring
        if self.step == ring.far:
            return
        if after:
            self.r, self.l = lax.optimization_barrier((self.r, self.l, *after))[:2]
        self.mark = self.r
        self.step += 1
        self.r = ring.hop(self.r, int(self.flip))
        self.blocks.append(self.r)
        self.offsets.append(-self.sign * self.step)
        if self.step <= ring.near:
            self.l = ring.hop(self.l, 1 - int(self.flip))
            self.blocks.append(self.l)
            self.offsets.append(self.sign * self.step)

    def finish(self):
        while self.step < self.ring.far:
            self.advance()
        return self.blocks


def on_device(logits, filter_logits, expression, observed, gene_mask, slide_ids, true_counts):
    layers, cell_rows, spot_cols = logits.shape
    n = lax.axis_size("cell")
    spots = lax.axis_size("spot")
    cells_all = cell_rows * n
    xs = spots // 2
    width = expression.shape[1]
    widths = SETS if sum(SETS) == width and all(w % (16 * n) == 0 for w in SETS) else [width]
    early = EARLY
    starts = [sum(widths[:h]) for h in range(len(widths))]
    owns = [w // n for w in widths]
    unit = math.gcd(*widths)
    sets = len(widths)
    ring = Ring(n)
    spot = lax.axis_index("spot")
    blocks_at = [
        lax.rem(spot // 2 - dx + xs, xs) * 2 + (spot % 2 + dc) % 2
        for dx in range(xs)
        for dc in range(2)
    ]
    me = jnp.stack([jnp.asarray(ring.place, jnp.int32)[lax.axis_index("cell")], *blocks_at])

    def send(v, dx, dc):
        pairs = []
        for s in range(spots):
            x, c = s // 2, s % 2
            pairs.append((s, ((x + dx) % xs) * 2 + (c ^ dc)))
        return lax.ppermute(v, "spot", pairs)

    expr, far = {}, {}
    held = expression
    for h in range(sets):
        piece = held[:, starts[h] : starts[h] + widths[h]]
        held = tie(expression, piece)
        for dx in range(1, xs):
            far[dx, h] = send(piece, dx, 0)
    partner = send(expression, 0, 1)
    for h in range(sets):
        col = starts[h] // widths[h]
        expr[0, 0, h] = (expression, col, widths[h])
        expr[0, 1, h] = (partner, col, widths[h])

    kept = jax.nn.sigmoid(filter_logits)
    entropy = jnp.sum(
        kept * jax.nn.softplus(-filter_logits) + (1.0 - kept) * jax.nn.softplus(filter_logits)
    ).reshape(1)

    hi, lo, sums = prep(logits, kept)

    def project(chosen, dxs, after=(), sums=None):
        parts = [
            (expr[dx, dc, h][0], expr[dx, dc, h][1] * widths[h], widths[h])
            for h in chosen
            for dx in dxs
            for dc in range(2)
        ]
        return forward(n, unit, me, tie(hi, *after) if after else hi, lo, parts, sums)

    def begin_far(h, after):
        for dx in range(1, xs):
            piece = tie(far[dx, h], after)
            expr[dx, 0, h] = (piece, 0, widths[h])
            expr[dx, 1, h] = (send(piece, 0, 1), 0, widths[h])

    away = range(1, xs)
    out = project(range(sets), [0], sums=sums)
    near = Scatter(ring, out, False)
    near.hop()
    slab, units = deal(ring, unit, me, tie(observed, near.mark), gene_mask)
    near.advance()
    begin_far(0, near.mark)
    near.advance()
    out = project([0], away, (near.mark,))
    rings = [Scatter(ring, out, True)]
    near.advance(out[0])
    rings[0].hop()
    near.finish()
    totals = near.r

    ids = slide_ids.reshape(1, spot_cols)
    extra = jnp.broadcast_to(
        jnp.pad(true_counts.astype(F32), (0, 8 - SLIDES), constant_values=1.0)[:, None],
        (8, 2 * xs * owns[0]),
    )
    shifts = [(dx, dc) for dx in range(xs) for dc in range(2)]
    gathers = []
    aux = None

    def begin(h, after):
        begin_far(h, after)
        out = project([h], away, (after,))
        rings.append(Scatter(ring, out, h % 2 == 0))
        return out[0]

    for h in range(sets):
        first, last = h == 0, h == sets - 1
        mine = rings[h]
        while mine.step < ring.far - 1:
            mine.advance()
            for g in gathers:
                g.advance()
        if not last and early[h]:
            out = begin(h + 1, mine.mark)
            mine.advance(out)
            rings[h + 1].hop()
        mine.finish()
        dealt = Dealt(
            units, width // unit, starts[h] // unit, widths[h] // unit, unit // n, layers, 2 * xs
        )
        at = [
            (sum(2 * owns[i] for i in range(h)), 2 * owns[h]),
            (0, 2 * (xs - 1) * owns[h]),
        ]
        qs = [near.r, mine.r]
        st = stats(dealt, me, ids, totals, slab, qs, at, first)
        sts = [st] + [send(st, dx, dc) for dx, dc in shifts[1:]]
        gp, extra = grads(
            shifts, dealt, xs, me, entropy, ids, totals, slab, extra, sts, qs, at, first, last
        )
        if first:
            aux = extra
        gathers.append(Gather(ring, gp, h % 2 == 0))
        gathers[-1].advance()
        if not last and not early[h]:
            begin(h + 1, gp)
            rings[h + 1].hop()
    tail = gathers[-1]
    parts = 2 if cell_rows % 512 == 0 else 1
    prior = [[] for _ in range(parts)]
    mark = tail.mark
    for h in range(sets - 1):
        blocks = gathers[h].finish()
        exprs = [expr[dx, dc, h] for dx in range(xs) for dc in range(2)]
        for j in range(parts):
            share = cell_rows // parts
            prior[j] = [
                backward_first(
                    n,
                    unit,
                    gathers[h].offsets,
                    tie(me, mark),
                    prior[j],
                    blocks,
                    exprs,
                    j * share,
                    share,
                )
            ]
            mark = tail.r
            tail.advance(prior[j][0])
    blocks, offsets = tail.finish(), tail.offsets
    exprs = [expr[dx, dc, sets - 1] for dx in range(xs) for dc in range(2)]
    grad_logits, filt = backward_last(
        n,
        unit,
        offsets,
        float(cells_all * G),
        me,
        logits,
        kept,
        totals,
        aux,
        [p for ps in prior for p in ps],
        blocks,
        exprs,
    )
    tails = sum(b[-8:] for b in blocks)
    count_terms = jnp.stack([aux[8 : 8 + SLIDES, l * spot_cols] for l in range(layers)])
    loss = jnp.sum(tails[1]) + jnp.sum(count_terms) + ENTROPY_WEIGHT * tails[-1, 0] / cells_all
    filt = filt.reshape(layers, cell_rows)
    grad_kept = filt
    for dx, dc in shifts[1:]:
        grad_kept = grad_kept + send(filt, dx, dc)
    slope = kept * (1.0 - kept)
    grad_filter = cells_all * (grad_kept * slope - ENTROPY_WEIGHT * slope * filter_logits / cells_all)
    return (grad_logits, grad_filter, count_terms, loss)


def solution(mesh):
    in_specs = (
        P(None, "cell", "spot"),
        P(None, "cell"),
        P("cell", "spot"),
        P(None, "cell", "spot"),
        P(None, "cell"),
        P("spot"),
        P(),
    )
    out_specs = (P(None, "cell", "spot"), P(None, "cell"), P(), P())
    return jax.shard_map(
        on_device, mesh=mesh, in_specs=in_specs, out_specs=out_specs, check_vma=False
    )
```

```python
import functools
import math

import jax
import jax.numpy as jnp
from jax import lax
from jax.experimental import pallas as pl
from jax.experimental.pallas import tpu as pltpu
from jax.sharding import PartitionSpec as P

G = 2048
SLIDES = 4
COUNT_WEIGHT = 0.0625
ENTROPY_WEIGHT = 1.0
EPSILON = 1e-06
COST = pl.CostEstimate(flops=1, bytes_accessed=1, transcendentals=0)
SETS = [256, 256]
F32 = jnp.float32
BF16 = jnp.bfloat16
NN = (((1,), (0,)), ((), ()))
NT = (((1,), (1,)), ((), ()))
TN = (((0,), (0,)), ((), ()))


def ring_order(n):
    if n < 8:
        return list(range(n))
    ys = math.isqrt(n // 2)
    zs = n // ys
    walk = [(z, 0) for z in range(zs)]
    for i, z in enumerate(reversed(range(zs))):
        cols = range(1, ys)
        walk += [(z, y) for y in (cols if i % 2 == 0 else reversed(cols))]
    return [z * ys + y for z, y in walk]


def split(v):
    hi = v.astype(BF16)
    return hi, (v - hi.astype(F32)).astype(BF16)


def mm(a, b, dims=NN):
    return lax.dot_general(a, b, dims, preferred_element_type=F32)


def mm_onehot(onehot, v, dims):
    hi, lo = split(v)
    if dims is TN:
        return mm(hi, onehot, dims) + mm(lo, onehot, dims)
    return mm(onehot, hi, dims) + mm(onehot, lo, dims)


def row_tile(rows):
    return rows // 2 if rows % 256 == 0 else rows


class Clock:
    def __init__(self, token):
        self.token = token

    def after(self, *vs):
        *vs, self.token = lax.optimization_barrier((*vs, self.token))
        return vs


def prep_kernel(x_ref, kept_ref, hi_ref, lo_ref, sum_ref):
    i = pl.program_id(1)
    e = jnp.exp(x_ref[0])
    rows, cols = e.shape
    kept = jnp.transpose(jnp.broadcast_to(kept_ref[0], (128, rows)))
    u = e * jnp.tile(kept, (1, cols // 128))

    @pl.when(i == 0)
    def _():
        sum_ref[...] = jnp.zeros_like(sum_ref)

    sum_ref[0, 0:1, :] += jnp.sum(e, axis=0, keepdims=True)
    sum_ref[0, 1:2, :] += jnp.sum(u, axis=0, keepdims=True)
    hi, lo = split(jnp.transpose(u))
    hi_ref[...] = hi
    lo_ref[...] = lo


def prep(x, kept):
    layers, rows, cols = x.shape
    tile = row_tile(rows)
    wide = pl.BlockSpec((cols, tile), lambda l, i: (l, i))
    return pl.pallas_call(
        prep_kernel,
        grid=(layers, rows // tile),
        in_specs=[
            pl.BlockSpec((1, tile, cols), lambda l, i: (l, i, 0)),
            pl.BlockSpec((1, 1, tile), lambda l, i: (l, 0, i)),
        ],
        out_specs=[wide, wide, pl.BlockSpec((1, 8, cols), lambda l, i: (l, 0, 0))],
        out_shape=[
            jax.ShapeDtypeStruct((layers * cols, rows), BF16),
            jax.ShapeDtypeStruct((layers * cols, rows), BF16),
            jax.ShapeDtypeStruct((layers, 8, cols), F32),
        ],
        name="prep",
        cost_estimate=COST,
    )(x, kept.reshape(layers, 1, rows))


def fwd_kernel(n, unit, cols, has_sums, me_ref, hi_hbm, lo_hbm, *refs):
    exprs, refs = refs[: len(cols)], refs[len(cols) :]
    sums_ref, refs = (refs[0], refs[1:]) if has_sums else (None, refs)
    outs, (hi, lo, expr, acc, turn, sems) = refs[:n], refs[n:]
    steps, chunk, genes = expr.shape

    def copies(i):
        at = pl.ds(pl.multiple_of(i * chunk, chunk), chunk)
        todo = [
            pltpu.make_async_copy(hi_hbm.at[:, at], hi.at[i], sems.at[0, i]),
            pltpu.make_async_copy(lo_hbm.at[:, at], lo.at[i], sems.at[1, i]),
        ]
        to = 0
        for j, (e, (col, w)) in enumerate(zip(exprs, cols)):
            todo.append(
                pltpu.make_async_copy(
                    e.at[at, col : col + w], expr.at[i, :, to : to + w], sems.at[2 + j, i]
                )
            )
            to += w
        return todo

    def start(i, carry):
        for c in copies(i):
            c.start()
        return carry

    def multiply(i, carry):
        for c in copies(i):
            c.wait()
        eh, el = split(expr[i])
        part = mm(hi[i], eh) + mm(lo[i], eh) + mm(hi[i], el)
        acc[...] = jnp.where(i == 0, part, acc[...] + part)
        return carry

    lax.fori_loop(0, steps, start, 0)
    lax.fori_loop(0, steps, multiply, 0)
    own = unit // n
    row = 0
    for at in range(0, genes, unit):
        turn[...] = jnp.transpose(acc[:, at : at + unit])
        for d in range(n):
            p = lax.rem(me_ref[0] + d, n)
            outs[d][row : row + own, :] = turn[pl.ds(pl.multiple_of(p * own, own), own), :]
        row += own
    if has_sums:
        layers, _, lanes = sums_ref.shape
        for d in range(n):
            for l in range(layers):
                outs[d][row : row + 8, l * lanes : (l + 1) * lanes] = sums_ref[l]


def forward(n, unit, me, hi, lo, exprs, sums=None):
    wide, rows = hi.shape
    chunk = 256 if rows % 256 == 0 else rows
    steps = rows // chunk
    genes = sum(w for _, _, w in exprs)
    out_rows = genes // n + (8 if sums is not None else 0)
    anywhere = pl.BlockSpec(memory_space=pl.ANY)
    in_specs = [pl.BlockSpec(memory_space=pltpu.SMEM)] + [anywhere] * (2 + len(exprs))
    args = [me, hi, lo] + [e for e, _, _ in exprs]
    if sums is not None:
        in_specs.append(pl.BlockSpec(memory_space=pltpu.VMEM))
        args.append(sums)
    cols = [(c, w) for _, c, w in exprs]
    return pl.pallas_call(
        functools.partial(fwd_kernel, n, unit, cols, sums is not None),
        in_specs=in_specs,
        out_shape=[jax.ShapeDtypeStruct((out_rows, wide), F32)] * n,
        scratch_shapes=[
            pltpu.VMEM((steps, wide, chunk), BF16),
            pltpu.VMEM((steps, wide, chunk), BF16),
            pltpu.VMEM((steps, chunk, genes), F32),
            pltpu.VMEM((wide, genes), F32),
            pltpu.VMEM((unit, wide), F32),
            pltpu.SemaphoreType.DMA((2 + len(exprs), steps)),
        ],
        name="fwd",
        cost_estimate=COST,
    )(*args)


def deal_kernel(place, unit, obs_ref, mask_ref, out_ref):
    n = len(place)
    layers, rows, _ = obs_ref.shape
    own, units = unit // n, rows // unit
    cut = layers * units * own
    out_ref[:, cut:, :] = jnp.zeros((n, out_ref.shape[1] - cut, out_ref.shape[2]), F32)
    for j in range(n):
        for u in range(units):
            src = slice(u * unit + place[j] * own, u * unit + (place[j] + 1) * own)
            for l in range(layers):
                to = (l * units + u) * own
                out_ref[j, to : to + own, :] = obs_ref[l, src, :]
            slides = mask_ref.shape[0]
            out_ref[j, cut + 8 * u : cut + 8 * u + slides, 0:own] = mask_ref[:, src].astype(F32)


def deal(ring, unit, clock, observed, gene_mask):
    layers, rows, cols = observed.shape
    n, own = ring.n, unit // ring.n
    if rows % unit:
        observed = lax.all_gather(observed, "cell", axis=1, tiled=True)
        gene_mask = lax.all_gather(gene_mask, "cell", axis=1, tiled=True)
        units = observed.shape[1] // unit
        pick = lambda a, at: lax.dynamic_index_in_dim(a, clock.token[0], at, keepdims=False)
        obs = pick(observed.reshape(layers, units, n, own, cols), 2)
        mask = pick(gene_mask.astype(F32).reshape(-1, units, n, own), 2).transpose(1, 0, 2)
        mask = jnp.pad(mask, ((0, 0), (0, 8 - mask.shape[1]), (0, cols - own)))
        slab = jnp.concatenate([obs.reshape(-1, cols), mask.reshape(-1, cols)])
        return slab[None], units
    units = rows // unit
    (gene_mask,) = clock.after(gene_mask)
    out = pl.pallas_call(
        functools.partial(deal_kernel, ring.place, unit),
        out_shape=jax.ShapeDtypeStruct((n, layers * units * own + 8 * units, cols), F32),
        name="deal",
    )(observed, gene_mask)
    (out,) = clock.after(out)
    return lax.all_to_all(out, "cell", 0, 0, tiled=True), units


def slide_rows(ids_ref, cols):
    return lax.broadcasted_iota(jnp.int32, (8, cols), 0) == ids_ref[...]


def held_rows(qs, at, lane, inv):
    return jnp.concatenate([q[r : r + rows, lane] for q, (r, rows) in zip(qs, at)], 0) * inv[:, lane]


class Dealt:
    def __init__(self, units, block_units, first, count, own, layers, blocks):
        self.units, self.block_units = units, block_units
        self.first, self.count, self.own = first, count, own
        self.layers, self.blocks = layers, blocks

    def places(self, me_ref):
        for j in range(self.blocks):
            for u in range(self.first, self.first + self.count):
                unit = me_ref[1 + j] * self.block_units + u
                yield unit // self.units, unit % self.units

    def obs(self, me_ref, slab_ref, l):
        rows = [
            slab_ref[s, pl.ds(pl.multiple_of((l * self.units + u) * self.own, self.own), self.own), :]
            for s, u in self.places(me_ref)
        ]
        return jnp.concatenate(rows, 0)

    def mask(self, me_ref, slab_ref):
        cut = self.layers * self.units * self.own
        cols = [
            slab_ref[s, pl.ds(pl.multiple_of(cut + 8 * u, 8), 8), 0 : self.own]
            for s, u in self.places(me_ref)
        ]
        return jnp.concatenate(cols, 1)


def stats_kernel(dealt, at, first, me_ref, ids_ref, tot_ref, slab_ref, *refs):
    qs, out_ref = refs[:-1], refs[-1]
    cols = ids_ref.shape[1]
    layers = tot_ref.shape[1] // cols
    onehot = slide_rows(ids_ref, cols).astype(F32)
    marks = onehot.astype(BF16)
    inv = 1.0 / tot_ref[-8:-7, :]
    for l in range(layers):
        lane = slice(l * cols, (l + 1) * cols)
        proj = held_rows(qs, at, lane, inv)
        obs = dealt.obs(me_ref, slab_ref, l)
        out_ref[24 * l : 24 * l + 8, :] = mm_onehot(marks, proj * obs, NT)
        out_ref[24 * l + 8 : 24 * l + 16, :] = mm_onehot(marks, proj * proj, NT)
        out_ref[24 * l + 16 : 24 * l + 24, :] = mm_onehot(marks, obs * obs, NT)
        if first:
            mass = onehot * (tot_ref[-7:-6, lane] * inv[:, lane])
            row = 24 * layers + 8 * l
            out_ref[row : row + 8, :] = jnp.broadcast_to(
                jnp.sum(mass, axis=1, keepdims=True), (8, out_ref.shape[1])
            )


SMEM_VMEM = lambda smem, vmem: [pl.BlockSpec(memory_space=pltpu.SMEM)] * smem + [
    pl.BlockSpec(memory_space=pltpu.VMEM)
] * vmem


def stats(dealt, me, ids, totals, slab, qs, at, first):
    layers = totals.shape[1] // ids.shape[1]
    genes = sum(r for _, r in at)
    return pl.pallas_call(
        functools.partial(stats_kernel, dealt, at, first),
        in_specs=SMEM_VMEM(1, 3 + len(qs)),
        out_shape=jax.ShapeDtypeStruct(((32 if first else 24) * layers, genes), F32),
        name="stats",
    )(me, ids, totals, slab, *qs)


def swap_lanes(v, group, shift):
    count, size = group
    run = count * size
    out = []
    for base in range(0, v.shape[1], run):
        for i in range(count):
            j = (i - shift) % count
            out.append(v[:, base + j * size : base + (j + 1) * size])
    return jnp.concatenate(out, 1)


def grad_kernel(shifts, dealt, at, xs, first, me_ref, ent_ref, *refs):
    ids_ref, tot_ref, slab_ref, extra_ref = refs[:4]
    refs = refs[4:]
    st_refs, refs = refs[: len(shifts)], refs[len(shifts) :]
    qs, (out_ref, aux_ref) = refs[:-2], refs[-2:]
    cols = ids_ref.shape[1]
    layers = tot_ref.shape[1] // cols
    genes = st_refs[0].shape[1]
    own = genes // (2 * xs)
    onehot = slide_rows(ids_ref, cols).astype(F32)
    marks = onehot.astype(BF16)
    inv = 1.0 / tot_ref[-8:-7, :]
    st = None
    for (dx, dc), ref in zip(shifts, st_refs):
        v = ref[...]
        if dc:
            v = swap_lanes(v, (2, own), 1)
        if dx:
            v = swap_lanes(v, (xs, 2 * own), dx)
        st = v if st is None else st + v
    mask = dealt.mask(me_ref, slab_ref)
    aux_ref[...] = jnp.zeros_like(aux_ref)
    out_rows = out_ref.shape[0]
    if out_rows > genes:
        out_ref[genes:out_rows, :] = jnp.full((out_rows - genes, layers * cols), ent_ref[0], F32)
    for l in range(layers):
        lane = slice(l * cols, (l + 1) * cols)
        cross = st[24 * l : 24 * l + 8]
        inv_proj = lax.rsqrt(st[24 * l + 8 : 24 * l + 16] + EPSILON)
        inv_obs = lax.rsqrt(st[24 * l + 16 : 24 * l + 24] + EPSILON)
        weight = mask * (-1.0 / G)
        term = jnp.sum(weight * (cross * inv_proj * inv_obs), axis=0, keepdims=True)
        spread_first = mm_onehot(marks, weight * inv_proj * inv_obs, TN)
        spread_second = mm_onehot(
            marks, weight * cross * (inv_proj * inv_proj * inv_proj) * inv_obs, TN
        )
        proj = held_rows(qs, at, lane, inv)
        grad = spread_first * dealt.obs(me_ref, slab_ref, l) - spread_second * proj
        out_ref[0:genes, lane] = grad
        back = jnp.sum(grad * proj, axis=0, keepdims=True)
        term = jnp.concatenate([term, jnp.zeros((1, cols - genes), F32)], 1)
        if first:
            mass = st[24 * layers + 8 * l : 24 * layers + 8 * l + 8]
            counts = extra_ref[:, :genes]
            off = (mass - counts) / counts
            slope = 2.0 * COUNT_WEIGHT * (mass - counts) / (counts * counts)
            aux_ref[1:2, lane] = jnp.sum(onehot * slope[:, 0:1], axis=0, keepdims=True)
            aux_ref[8:16, l * cols : l * cols + genes] = COUNT_WEIGHT * (off * off)
        else:
            back = back + extra_ref[0:1, lane]
            term = term + extra_ref[2:3, lane]
        aux_ref[0:1, lane] = back
        aux_ref[2:3, lane] = term
        if out_rows > genes:
            out_ref[genes : genes + 1, lane] = back
            out_ref[genes + 1 : genes + 2, lane] = term


def grads(shifts, dealt, xs, me, ent, ids, totals, slab, extra, sts, qs, at, first, last):
    genes, wide = sum(r for _, r in at), totals.shape[1]
    return pl.pallas_call(
        functools.partial(grad_kernel, shifts, dealt, at, xs, first),
        in_specs=SMEM_VMEM(2, 4 + len(sts) + len(qs)),
        out_shape=[
            jax.ShapeDtypeStruct((genes + (8 if last else 0), wide), F32),
            jax.ShapeDtypeStruct((16, wide), F32),
        ],
        name="grads",
    )(me, ent, ids, totals, slab, extra, *sts, *qs)


def gather_rows(n, unit, me_ref, offsets, blocks, hi, lo):
    own = unit // n
    for d, block in zip(offsets, blocks):
        p = lax.rem(me_ref[0] + d + n, n)
        for j in range(hi.shape[0] // unit):
            h, lw = split(block[j * own : (j + 1) * own, :])
            at = pl.ds(pl.multiple_of(j * unit + p * own, own), own)
            hi[at, :] = h
            lo[at, :] = lw


def product(exprs, hi, lo, lanes):
    eh, el = split(jnp.concatenate([e[...] for e in exprs], 1))
    gh, gl = hi[:, lanes], lo[:, lanes]
    return mm(eh, gh) + mm(eh, gl) + mm(el, gh)


def bwd_first_kernel(n, unit, offsets, priors, me_ref, *refs):
    out_ref, hi, lo = refs[-3:]
    prior, refs = refs[:priors], refs[priors:]
    blocks = refs[: len(offsets)]
    exprs = refs[len(offsets) : -3]

    @pl.when(pl.program_id(0) == 0)
    def _():
        gather_rows(n, unit, me_ref, offsets, blocks, hi, lo)

    total = product(exprs, hi, lo, slice(None))
    for p in prior:
        total = total + p[...]
    out_ref[...] = total


def bwd_last_kernel(n, unit, offsets, scale, splits, me_ref, *refs):
    x_ref, kept_ref, tot_ref, aux_ref = refs[:4]
    refs = refs[4:]
    priors, refs = refs[: len(splits)], refs[len(splits) :]
    grad_ref, filt_ref, hi, lo, back = refs[-5:]
    blocks = refs[: len(offsets)]
    exprs = refs[len(offsets) : -5]
    layers, rows, cols = x_ref.shape

    @pl.when(pl.program_id(0) == 0)
    def _():
        gather_rows(n, unit, me_ref, offsets, blocks, hi, lo)
        total = blocks[0][-8:, :]
        for b in blocks[1:]:
            total += b[-8:, :]
        back[...] = total
        for l in range(layers):
            lane = slice(l * cols, (l + 1) * cols)
            inv = 1.0 / tot_ref[-8:-7, lane]
            mass = tot_ref[-7:-6, lane] * inv
            back[2:3, lane] = inv
            back[3:4, lane] = total[0:1, lane] + aux_ref[1:2, lane] * mass

    for l in range(layers):
        lane = slice(l * cols, (l + 1) * cols)
        gw = product(exprs, hi, lo, lane)
        if splits:
            held = [p[:, lane] for p in priors]
            gw = gw + functools.reduce(
                lambda low, j: jnp.where(pl.program_id(0) < splits[j], low, held[j]),
                range(1, len(held)),
                held[0],
            )
        gw = gw + aux_ref[1:2, lane]
        mapping = jnp.exp(x_ref[l]) * back[2:3, lane]
        kept = jnp.transpose(jnp.broadcast_to(kept_ref[l], (128, rows)))
        kept = jnp.tile(kept, (1, cols // 128))
        grad_ref[l] = scale * (mapping * (kept * gw - back[3:4, lane]))
        share = mapping * gw
        lanes = share[:, 0:128]
        for c in range(128, cols, 128):
            lanes = lanes + share[:, c : c + 128]
        filt_ref[l] = jnp.sum(jnp.transpose(lanes), axis=0, keepdims=True)


def backward_first(n, unit, offsets, me, prior, blocks, exprs, begin, rows):
    tile = 256 if rows % 256 == 0 else rows
    wide = blocks[0].shape[1]
    genes = sum(w for _, _, w in exprs)
    skip = begin // tile
    whole = pl.BlockSpec(blocks[0].shape, lambda i: (0, 0))
    return pl.pallas_call(
        functools.partial(bwd_first_kernel, n, unit, offsets, len(prior)),
        grid=(rows // tile,),
        in_specs=[pl.BlockSpec(memory_space=pltpu.SMEM)]
        + [pl.BlockSpec((tile, wide), lambda i: (i, 0))] * len(prior)
        + [whole] * len(blocks)
        + [pl.BlockSpec((tile, w), lambda i, c=c: (i + skip, c)) for _, c, w in exprs],
        out_specs=pl.BlockSpec((tile, wide), lambda i: (i, 0)),
        out_shape=jax.ShapeDtypeStruct((rows, wide), F32),
        scratch_shapes=[pltpu.VMEM((genes, wide), BF16), pltpu.VMEM((genes, wide), BF16)],
        name="bwd_first",
        cost_estimate=COST,
    )(me, *prior, *blocks, *[e for e, _, _ in exprs])


def backward_last(n, unit, offsets, scale, me, x, kept, totals, aux, prior, blocks, exprs):
    tile = 256
    layers, rows, cols = x.shape
    wide = layers * cols
    genes = sum(w for _, _, w in exprs)
    fixed = lambda a: pl.BlockSpec(a.shape, lambda i: (0,) * a.ndim)
    args = [me, x, kept.reshape(layers, 1, rows), totals, aux]
    in_specs = [
        pl.BlockSpec(memory_space=pltpu.SMEM),
        pl.BlockSpec((layers, tile, cols), lambda i: (0, i, 0)),
        pl.BlockSpec((layers, 1, tile), lambda i: (0, 0, i)),
        fixed(totals),
        fixed(aux),
    ]
    args += prior
    splits = []
    for p in prior:
        begin = splits[-1] + prior[len(splits) - 1].shape[0] // tile if splits else 0
        splits.append(begin)
        steps = p.shape[0] // tile
        in_specs.append(
            pl.BlockSpec(
                (tile, wide), lambda i, b=begin, t=steps: (jnp.clip(i - b, 0, t - 1), 0)
            )
        )
    args += list(blocks) + [e for e, _, _ in exprs]
    in_specs += [fixed(b) for b in blocks]
    in_specs += [pl.BlockSpec((tile, w), lambda i, c=c: (i, c)) for _, c, w in exprs]
    return pl.pallas_call(
        functools.partial(bwd_last_kernel, n, unit, offsets, scale, splits),
        grid=(rows // tile,),
        in_specs=in_specs,
        out_specs=[
            pl.BlockSpec((layers, tile, cols), lambda i: (0, i, 0)),
            pl.BlockSpec((layers, 1, tile), lambda i: (0, 0, i)),
        ],
        out_shape=[
            jax.ShapeDtypeStruct((layers, rows, cols), F32),
            jax.ShapeDtypeStruct((layers, 1, rows), F32),
        ],
        scratch_shapes=[
            pltpu.VMEM((genes, wide), BF16),
            pltpu.VMEM((genes, wide), BF16),
            pltpu.VMEM((8, wide), F32),
        ],
        name="bwd_last",
        cost_estimate=COST,
    )(*args)


class Ring:
    def __init__(self, n):
        self.n = n
        order = ring_order(n)
        self.place = [order.index(i) for i in range(n)]
        right = [(order[i], order[(i + 1) % n]) for i in range(n)]
        self.dirs = (right, [(b, a) for a, b in right])
        self.far = n // 2
        self.near = n - 1 - self.far

    def hop(self, v, way):
        return lax.ppermute(v, "cell", self.dirs[way])


class Scatter:
    def __init__(self, ring, clock, v, flip):
        self.ring, self.clock, self.v, self.flip = ring, clock, v, flip
        self.sign = -1 if flip else 1
        self.step = 0
        self.r, self.l = self.at(ring.far), self.at(-ring.near)
        self.hop()

    def at(self, d):
        return self.v[(self.sign * d) % self.ring.n]

    def hop(self):
        self.r = self.ring.hop(self.r, int(self.flip))
        if self.step < self.ring.near:
            self.l = self.ring.hop(self.l, 1 - int(self.flip))
        self.step += 1

    def wait(self):
        self.r, self.l = self.clock.after(self.r, self.l)

    def advance(self):
        ring, s = self.ring, self.step - 1
        if s < ring.far - 1:
            self.r = self.r + self.at(ring.far - 1 - s)
        if s < ring.near - 1:
            self.l = self.l + self.at(s + 1 - ring.near)
        if self.step == ring.far:
            self.r = self.r + self.l + self.at(0)
        if self.step < ring.near:
            self.r, self.l = self.clock.after(self.r, self.l)
        else:
            (self.r,) = self.clock.after(self.r)
        if self.step < ring.far:
            self.hop()
            return True
        return False


class Gather:
    def __init__(self, ring, clock, v, flip):
        self.ring, self.clock, self.flip = ring, clock, flip
        self.sign = -1 if flip else 1
        self.blocks, self.offsets = [v], [0]
        self.r = self.l = v
        self.step = 0
        self.hop()

    def hop(self):
        self.step += 1
        self.r = self.ring.hop(self.r, int(self.flip))
        if self.step <= self.ring.near:
            self.l = self.ring.hop(self.l, 1 - int(self.flip))

    def wait(self):
        if self.step <= self.ring.near:
            self.r, self.l = self.clock.after(self.r, self.l)
        else:
            (self.r,) = self.clock.after(self.r)

    def advance(self):
        ring = self.ring
        self.blocks.append(self.r)
        self.offsets.append(-self.sign * self.step)
        if self.step <= ring.near:
            self.blocks.append(self.l)
            self.offsets.append(self.sign * self.step)
        if self.step < ring.far:
            self.hop()
            return True
        return False


def slot(*chains):
    for c in chains:
        c.wait()
    return any([c.advance() for c in chains])


def finish(chain):
    while slot(chain):
        pass


def on_device(logits, filter_logits, expression, observed, gene_mask, slide_ids, true_counts):
    layers, cell_rows, spot_cols = logits.shape
    n = lax.axis_size("cell")
    spots = lax.axis_size("spot")
    cells_all = cell_rows * n
    xs = spots // 2
    width = expression.shape[1]
    widths = SETS if sum(SETS) == width and all(w % (16 * n) == 0 for w in SETS) else [width]
    starts = [sum(widths[:h]) for h in range(len(widths))]
    owns = [w // n for w in widths]
    unit = math.gcd(*widths)
    sets = len(widths)
    ring = Ring(n)
    table = [
        [place] + [(q // 2 - dx) % xs * 2 + (q + dc) % 2 for dx in range(xs) for dc in range(2)]
        for place in ring.place
        for q in range(spots)
    ]
    me = lax.dynamic_index_in_dim(
        jnp.asarray(table, jnp.int32), lax.axis_index(("cell", "spot")), keepdims=False
    )

    def send(v, dx, dc):
        pairs = []
        for s in range(spots):
            x, c = s // 2, s % 2
            pairs.append((s, ((x + dx) % xs) * 2 + (c ^ dc)))
        return lax.ppermute(v, "spot", pairs)

    expr, far = {}, {}
    clock = Clock(me)

    def begin_x(h):
        (held,) = clock.after(expression)
        (piece,) = clock.after(held[:, starts[h] : starts[h] + widths[h]])
        for dx in range(1, xs):
            far[dx, h] = send(piece, dx, 0)

    begin_x(0)
    partner = send(clock.after(expression)[0], 0, 1)
    for h in range(sets):
        col = starts[h] // widths[h]
        expr[0, 0, h] = (expression, col, widths[h])
        expr[0, 1, h] = (partner, col, widths[h])

    kept = jax.nn.sigmoid(filter_logits)
    slab, units = deal(ring, unit, clock, observed, gene_mask)
    (kept,) = clock.after(kept)
    hi, lo, sums = prep(logits, kept)
    hi, lo, sums = clock.after(hi, lo, sums)
    away = range(1, xs)

    def project(chosen, dxs, flip, sums=None):
        parts = [
            (expr[dx, dc, h][0], expr[dx, dc, h][1] * widths[h], widths[h])
            for h in chosen
            for dx in dxs
            for dc in range(2)
        ]
        out = forward(n, unit, clock.token, hi, lo, parts, sums)
        out = clock.after(*out)
        return Scatter(ring, clock, out, flip)

    def begin_far(h):
        for dx in range(1, xs):
            (piece,) = clock.after(far[dx, h])
            expr[dx, 0, h] = (piece, 0, widths[h])
            expr[dx, 1, h] = (send(piece, 0, 1), 0, widths[h])

    ids = slide_ids.reshape(1, spot_cols)
    shifts = [(dx, dc) for dx in range(xs) for dc in range(2)]
    held = {
        "extra": jnp.broadcast_to(
            jnp.pad(true_counts.astype(F32), (0, 8 - SLIDES), constant_values=1.0)[:, None],
            (8, 2 * xs * owns[0]),
        )
    }

    def rows_of(h):
        at = Dealt(
            units, width // unit, starts[h] // unit, widths[h] // unit, unit // n, layers, 2 * xs
        )
        return at, [near[h].r, rings[h].r], [(0, 2 * owns[h]), (0, 2 * (xs - 1) * owns[h])]

    def take_stats(h):
        dealt, qs, at = rows_of(h)
        st = stats(dealt, clock.token, ids, near[0].r, slab, qs, at, h == 0)
        (st,) = clock.after(st)
        return [st] + [send(st, dx, dc) for dx, dc in shifts[1:]]

    def take_grads(h, sts):
        dealt, qs, at = rows_of(h)
        gp, more = grads(
            shifts,
            dealt,
            xs,
            clock.token,
            entropy,
            ids,
            near[0].r,
            slab,
            held["extra"],
            sts,
            qs,
            at,
            h == 0,
            h == sets - 1,
        )
        held["extra"] = more
        if h == 0:
            held["aux"] = more
        (gp,) = clock.after(gp)
        return Gather(ring, clock, gp, h % 2 == 0)

    if cell_rows % 256 == 0 and cell_rows > 256:
        cut = cell_rows // 512 * 256
        shares = [(0, cut), (cut, cell_rows - cut)]
    else:
        shares = [(0, cell_rows)]
    parts = len(shares)
    prior = [[] for _ in range(parts)]

    def multiply_back(h, j):
        prior[j] = [
            backward_first(
                n,
                unit,
                gathers[h].offsets,
                clock.token,
                prior[j],
                gathers[h].blocks,
                [expr[dx, dc, h] for dx in range(xs) for dc in range(2)],
                *shares[j],
            )
        ]
        prior[j] = clock.after(prior[j][0])

    rings, gathers = [], []
    near = [project([0], [0], False, sums)]
    (slab,) = clock.after(slab)
    scores, gates = clock.after(filter_logits, kept)
    entropy = jnp.sum(
        gates * jax.nn.softplus(-scores) + (1.0 - gates) * jax.nn.softplus(scores)
    ).reshape(1)
    for h in range(1, sets):
        near.append(project([h], [0], h % 2 == 1))
        begin_x(h)
    if sets == 2:
        slot(near[0])
        begin_far(0)
        rings.append(project([0], away, True))
        slot(near[0], near[1])
        slot(near[0], near[1], rings[0])
        slot(near[0], near[1], rings[0])
        begin_far(1)
        rings.append(project([1], away, False))
        slot(near[1], rings[0])
        slot(rings[0], rings[1])
        sts = take_stats(0)
        slot(rings[1])
        gathers.append(take_grads(0, sts))
        slot(rings[1], gathers[0])
        slot(rings[1], gathers[0])
        gathers.append(take_grads(1, take_stats(1)))
        slot(gathers[0])
        slot(gathers[0], gathers[1])
        for j in range(parts):
            multiply_back(0, j)
            slot(gathers[1])
        finish(gathers[1])
    else:
        for q in near:
            finish(q)
        for h in range(sets):
            begin_far(h)
            rings.append(project([h], away, True))
            finish(rings[h])
            gathers.append(take_grads(h, take_stats(h)))
            finish(gathers[h])
        for h in range(sets - 1):
            for j in range(parts):
                multiply_back(h, j)
    totals, aux = near[0].r, held["aux"]
    blocks, offsets = gathers[-1].blocks, gathers[-1].offsets
    exprs = [expr[dx, dc, sets - 1] for dx in range(xs) for dc in range(2)]
    grad_logits, filt = backward_last(
        n,
        unit,
        offsets,
        float(cells_all * G),
        clock.token,
        logits,
        kept,
        totals,
        aux,
        [p for ps in prior for p in ps],
        blocks,
        exprs,
    )
    tails = sum(b[-8:] for b in blocks)
    count_terms = jnp.stack([aux[8 : 8 + SLIDES, l * spot_cols] for l in range(layers)])
    loss = jnp.sum(tails[1]) + jnp.sum(count_terms) + ENTROPY_WEIGHT * tails[-1, 0] / cells_all
    filt = filt.reshape(layers, cell_rows)
    grad_kept = filt
    for dx, dc in shifts[1:]:
        grad_kept = grad_kept + send(filt, dx, dc)
    slope = kept * (1.0 - kept)
    grad_filter = cells_all * (grad_kept * slope - ENTROPY_WEIGHT * slope * filter_logits / cells_all)
    return (grad_logits, grad_filter, count_terms, loss)


def solution(mesh):
    in_specs = (
        P(None, "cell", "spot"),
        P(None, "cell"),
        P("cell", "spot"),
        P(None, "cell", "spot"),
        P(None, "cell"),
        P("spot"),
        P(),
    )
    out_specs = (P(None, "cell", "spot"), P(None, "cell"), P(), P())
    return jax.shard_map(
        on_device, mesh=mesh, in_specs=in_specs, out_specs=out_specs, check_vma=False
    )
```

```python
import functools
import math

import jax
import jax.numpy as jnp
from jax import lax
from jax.experimental import pallas as pl
from jax.experimental.pallas import tpu as pltpu
from jax.sharding import PartitionSpec as P

G = 2048
SLIDES = 4
COUNT_WEIGHT = 0.0625
ENTROPY_WEIGHT = 1.0
EPSILON = 1e-06
COST = pl.CostEstimate(flops=1, bytes_accessed=1, transcendentals=0)
SETS = [256, 256]
F32 = jnp.float32
BF16 = jnp.bfloat16
NN = (((1,), (0,)), ((), ()))
NT = (((1,), (1,)), ((), ()))
TN = (((0,), (0,)), ((), ()))


def ring_order(n):
    if n < 8:
        return list(range(n))
    ys = math.isqrt(n // 2)
    zs = n // ys
    walk = [(z, 0) for z in range(zs)]
    for i, z in enumerate(reversed(range(zs))):
        cols = range(1, ys)
        walk += [(z, y) for y in (cols if i % 2 == 0 else reversed(cols))]
    return [z * ys + y for z, y in walk]


def split(v):
    hi = v.astype(BF16)
    return hi, (v - hi.astype(F32)).astype(BF16)


def mm(a, b, dims=NN):
    return lax.dot_general(a, b, dims, preferred_element_type=F32)


def mm_onehot(onehot, v, dims):
    hi, lo = split(v)
    if dims is TN:
        return mm(hi, onehot, dims) + mm(lo, onehot, dims)
    return mm(onehot, hi, dims) + mm(onehot, lo, dims)


def row_tile(rows):
    return rows // 2 if rows % 256 == 0 else rows


class Clock:
    def __init__(self, token):
        self.token = token

    def after(self, *vs):
        *vs, self.token = lax.optimization_barrier((*vs, self.token))
        return vs


def prep_kernel(x_ref, kept_ref, hi_ref, lo_ref, sum_ref):
    i = pl.program_id(1)
    e = jnp.exp(x_ref[0])
    rows, cols = e.shape
    kept = jnp.transpose(jnp.broadcast_to(kept_ref[0], (128, rows)))
    u = e * jnp.tile(kept, (1, cols // 128))

    @pl.when(i == 0)
    def _():
        sum_ref[...] = jnp.zeros_like(sum_ref)

    sum_ref[0, 0:1, :] += jnp.sum(e, axis=0, keepdims=True)
    sum_ref[0, 1:2, :] += jnp.sum(u, axis=0, keepdims=True)
    hi, lo = split(jnp.transpose(u))
    hi_ref[...] = hi
    lo_ref[...] = lo


def prep(x, kept):
    layers, rows, cols = x.shape
    tile = row_tile(rows)
    wide = pl.BlockSpec((cols, tile), lambda l, i: (l, i))
    return pl.pallas_call(
        prep_kernel,
        grid=(layers, rows // tile),
        in_specs=[
            pl.BlockSpec((1, tile, cols), lambda l, i: (l, i, 0)),
            pl.BlockSpec((1, 1, tile), lambda l, i: (l, 0, i)),
        ],
        out_specs=[wide, wide, pl.BlockSpec((1, 8, cols), lambda l, i: (l, 0, 0))],
        out_shape=[
            jax.ShapeDtypeStruct((layers * cols, rows), BF16),
            jax.ShapeDtypeStruct((layers * cols, rows), BF16),
            jax.ShapeDtypeStruct((layers, 8, cols), F32),
        ],
        name="prep",
        cost_estimate=COST,
    )(x, kept.reshape(layers, 1, rows))


def fwd_kernel(n, unit, cols, has_sums, me_ref, hi_hbm, lo_hbm, *refs):
    exprs, refs = refs[: len(cols)], refs[len(cols) :]
    sums_ref, refs = (refs[0], refs[1:]) if has_sums else (None, refs)
    outs, (hi, lo, expr, acc, turn, sems) = refs[:n], refs[n:]
    steps, chunk, genes = expr.shape

    def copies(i):
        at = pl.ds(pl.multiple_of(i * chunk, chunk), chunk)
        todo = [
            pltpu.make_async_copy(hi_hbm.at[:, at], hi.at[i], sems.at[0, i]),
            pltpu.make_async_copy(lo_hbm.at[:, at], lo.at[i], sems.at[1, i]),
        ]
        to = 0
        for j, (e, (col, w)) in enumerate(zip(exprs, cols)):
            todo.append(
                pltpu.make_async_copy(
                    e.at[at, col : col + w], expr.at[i, :, to : to + w], sems.at[2 + j, i]
                )
            )
            to += w
        return todo

    def start(i, carry):
        for c in copies(i):
            c.start()
        return carry

    def multiply(i, carry):
        for c in copies(i):
            c.wait()
        eh, el = split(expr[i])
        part = mm(hi[i], eh) + mm(lo[i], eh) + mm(hi[i], el)
        acc[...] = jnp.where(i == 0, part, acc[...] + part)
        return carry

    lax.fori_loop(0, steps, start, 0)
    lax.fori_loop(0, steps, multiply, 0)
    own = unit // n
    row = 0
    for at in range(0, genes, unit):
        turn[...] = jnp.transpose(acc[:, at : at + unit])
        for d in range(n):
            p = lax.rem(me_ref[0] + d, n)
            outs[d][row : row + own, :] = turn[pl.ds(pl.multiple_of(p * own, own), own), :]
        row += own
    if has_sums:
        layers, _, lanes = sums_ref.shape
        for d in range(n):
            for l in range(layers):
                outs[d][row : row + 8, l * lanes : (l + 1) * lanes] = sums_ref[l]


def forward(n, unit, me, hi, lo, exprs, sums=None):
    wide, rows = hi.shape
    chunk = 256 if rows % 256 == 0 else rows
    steps = rows // chunk
    genes = sum(w for _, _, w in exprs)
    out_rows = genes // n + (8 if sums is not None else 0)
    anywhere = pl.BlockSpec(memory_space=pl.ANY)
    in_specs = [pl.BlockSpec(memory_space=pltpu.SMEM)] + [anywhere] * (2 + len(exprs))
    args = [me, hi, lo] + [e for e, _, _ in exprs]
    if sums is not None:
        in_specs.append(pl.BlockSpec(memory_space=pltpu.VMEM))
        args.append(sums)
    cols = [(c, w) for _, c, w in exprs]
    return pl.pallas_call(
        functools.partial(fwd_kernel, n, unit, cols, sums is not None),
        in_specs=in_specs,
        out_shape=[jax.ShapeDtypeStruct((out_rows, wide), F32)] * n,
        scratch_shapes=[
            pltpu.VMEM((steps, wide, chunk), BF16),
            pltpu.VMEM((steps, wide, chunk), BF16),
            pltpu.VMEM((steps, chunk, genes), F32),
            pltpu.VMEM((wide, genes), F32),
            pltpu.VMEM((unit, wide), F32),
            pltpu.SemaphoreType.DMA((2 + len(exprs), steps)),
        ],
        name="fwd",
        cost_estimate=COST,
    )(*args)


def deal_kernel(place, unit, obs_ref, mask_ref, out_ref):
    n = len(place)
    layers, rows, _ = obs_ref.shape
    own, units = unit // n, rows // unit
    cut = layers * units * own
    out_ref[:, cut:, :] = jnp.zeros((n, out_ref.shape[1] - cut, out_ref.shape[2]), F32)
    for j in range(n):
        for u in range(units):
            src = slice(u * unit + place[j] * own, u * unit + (place[j] + 1) * own)
            for l in range(layers):
                to = (l * units + u) * own
                out_ref[j, to : to + own, :] = obs_ref[l, src, :]
            slides = mask_ref.shape[0]
            out_ref[j, cut + 8 * u : cut + 8 * u + slides, 0:own] = mask_ref[:, src].astype(F32)


def deal(ring, unit, clock, observed, gene_mask):
    layers, rows, cols = observed.shape
    n, own = ring.n, unit // ring.n
    if rows % unit:
        observed = lax.all_gather(observed, "cell", axis=1, tiled=True)
        gene_mask = lax.all_gather(gene_mask, "cell", axis=1, tiled=True)
        units = observed.shape[1] // unit
        pick = lambda a, at: lax.dynamic_index_in_dim(a, clock.token[0], at, keepdims=False)
        obs = pick(observed.reshape(layers, units, n, own, cols), 2)
        mask = pick(gene_mask.astype(F32).reshape(-1, units, n, own), 2).transpose(1, 0, 2)
        mask = jnp.pad(mask, ((0, 0), (0, 8 - mask.shape[1]), (0, cols - own)))
        slab = jnp.concatenate([obs.reshape(-1, cols), mask.reshape(-1, cols)])
        return slab[None], units
    units = rows // unit
    (gene_mask,) = clock.after(gene_mask)
    out = pl.pallas_call(
        functools.partial(deal_kernel, ring.place, unit),
        out_shape=jax.ShapeDtypeStruct((n, layers * units * own + 8 * units, cols), F32),
        name="deal",
    )(observed, gene_mask)
    (out,) = clock.after(out)
    return lax.all_to_all(out, "cell", 0, 0, tiled=True), units


def slide_rows(ids_ref, cols):
    return lax.broadcasted_iota(jnp.int32, (8, cols), 0) == ids_ref[...]


def held_rows(qs, at, lane, inv):
    return jnp.concatenate([q[r : r + rows, lane] for q, (r, rows) in zip(qs, at)], 0) * inv[:, lane]


class Dealt:
    def __init__(self, units, block_units, first, count, own, layers, blocks):
        self.units, self.block_units = units, block_units
        self.first, self.count, self.own = first, count, own
        self.layers, self.blocks = layers, blocks

    def places(self, me_ref):
        for j in range(self.blocks):
            for u in range(self.first, self.first + self.count):
                unit = me_ref[1 + j] * self.block_units + u
                yield unit // self.units, unit % self.units

    def obs(self, me_ref, slab_ref, l):
        rows = [
            slab_ref[s, pl.ds(pl.multiple_of((l * self.units + u) * self.own, self.own), self.own), :]
            for s, u in self.places(me_ref)
        ]
        return jnp.concatenate(rows, 0)

    def mask(self, me_ref, slab_ref):
        cut = self.layers * self.units * self.own
        cols = [
            slab_ref[s, pl.ds(pl.multiple_of(cut + 8 * u, 8), 8), 0 : self.own]
            for s, u in self.places(me_ref)
        ]
        return jnp.concatenate(cols, 1)


def stats_kernel(dealt, at, first, me_ref, ids_ref, tot_ref, slab_ref, *refs):
    qs, out_ref = refs[:-1], refs[-1]
    cols = ids_ref.shape[1]
    layers = tot_ref.shape[1] // cols
    onehot = slide_rows(ids_ref, cols).astype(F32)
    marks = onehot.astype(BF16)
    inv = 1.0 / tot_ref[-8:-7, :]
    for l in range(layers):
        lane = slice(l * cols, (l + 1) * cols)
        proj = held_rows(qs, at, lane, inv)
        obs = dealt.obs(me_ref, slab_ref, l)
        out_ref[24 * l : 24 * l + 8, :] = mm_onehot(marks, proj * obs, NT)
        out_ref[24 * l + 8 : 24 * l + 16, :] = mm_onehot(marks, proj * proj, NT)
        out_ref[24 * l + 16 : 24 * l + 24, :] = mm_onehot(marks, obs * obs, NT)
        if first:
            mass = onehot * (tot_ref[-7:-6, lane] * inv[:, lane])
            row = 24 * layers + 8 * l
            out_ref[row : row + 8, :] = jnp.broadcast_to(
                jnp.sum(mass, axis=1, keepdims=True), (8, out_ref.shape[1])
            )


SMEM_VMEM = lambda smem, vmem: [pl.BlockSpec(memory_space=pltpu.SMEM)] * smem + [
    pl.BlockSpec(memory_space=pltpu.VMEM)
] * vmem


def stats(dealt, me, ids, totals, slab, qs, at, first):
    layers = totals.shape[1] // ids.shape[1]
    genes = sum(r for _, r in at)
    return pl.pallas_call(
        functools.partial(stats_kernel, dealt, at, first),
        in_specs=SMEM_VMEM(1, 3 + len(qs)),
        out_shape=jax.ShapeDtypeStruct(((32 if first else 24) * layers, genes), F32),
        name="stats",
    )(me, ids, totals, slab, *qs)


def swap_lanes(v, group, shift):
    count, size = group
    run = count * size
    out = []
    for base in range(0, v.shape[1], run):
        for i in range(count):
            j = (i - shift) % count
            out.append(v[:, base + j * size : base + (j + 1) * size])
    return jnp.concatenate(out, 1)


def grad_kernel(shifts, dealt, at, xs, first, me_ref, ent_ref, *refs):
    ids_ref, tot_ref, slab_ref, extra_ref = refs[:4]
    refs = refs[4:]
    st_refs, refs = refs[: len(shifts)], refs[len(shifts) :]
    qs, (out_ref, aux_ref) = refs[:-2], refs[-2:]
    cols = ids_ref.shape[1]
    layers = tot_ref.shape[1] // cols
    genes = st_refs[0].shape[1]
    own = genes // (2 * xs)
    onehot = slide_rows(ids_ref, cols).astype(F32)
    marks = onehot.astype(BF16)
    inv = 1.0 / tot_ref[-8:-7, :]
    st = None
    for (dx, dc), ref in zip(shifts, st_refs):
        v = ref[...]
        if dc:
            v = swap_lanes(v, (2, own), 1)
        if dx:
            v = swap_lanes(v, (xs, 2 * own), dx)
        st = v if st is None else st + v
    mask = dealt.mask(me_ref, slab_ref)
    aux_ref[...] = jnp.zeros_like(aux_ref)
    out_rows = out_ref.shape[0]
    if out_rows > genes:
        out_ref[genes:out_rows, :] = jnp.full((out_rows - genes, layers * cols), ent_ref[0], F32)
    for l in range(layers):
        lane = slice(l * cols, (l + 1) * cols)
        cross = st[24 * l : 24 * l + 8]
        inv_proj = lax.rsqrt(st[24 * l + 8 : 24 * l + 16] + EPSILON)
        inv_obs = lax.rsqrt(st[24 * l + 16 : 24 * l + 24] + EPSILON)
        weight = mask * (-1.0 / G)
        term = jnp.sum(weight * (cross * inv_proj * inv_obs), axis=0, keepdims=True)
        spread_first = mm_onehot(marks, weight * inv_proj * inv_obs, TN)
        spread_second = mm_onehot(
            marks, weight * cross * (inv_proj * inv_proj * inv_proj) * inv_obs, TN
        )
        proj = held_rows(qs, at, lane, inv)
        grad = spread_first * dealt.obs(me_ref, slab_ref, l) - spread_second * proj
        out_ref[0:genes, lane] = grad
        back = jnp.sum(grad * proj, axis=0, keepdims=True)
        term = jnp.concatenate([term, jnp.zeros((1, cols - genes), F32)], 1)
        if first:
            mass = st[24 * layers + 8 * l : 24 * layers + 8 * l + 8]
            counts = extra_ref[:, :genes]
            off = (mass - counts) / counts
            slope = 2.0 * COUNT_WEIGHT * (mass - counts) / (counts * counts)
            aux_ref[1:2, lane] = jnp.sum(onehot * slope[:, 0:1], axis=0, keepdims=True)
            aux_ref[8:16, l * cols : l * cols + genes] = COUNT_WEIGHT * (off * off)
        else:
            back = back + extra_ref[0:1, lane]
            term = term + extra_ref[2:3, lane]
        aux_ref[0:1, lane] = back
        aux_ref[2:3, lane] = term
        if out_rows > genes:
            out_ref[genes : genes + 1, lane] = back
            out_ref[genes + 1 : genes + 2, lane] = term


def grads(shifts, dealt, xs, me, ent, ids, totals, slab, extra, sts, qs, at, first, last):
    genes, wide = sum(r for _, r in at), totals.shape[1]
    return pl.pallas_call(
        functools.partial(grad_kernel, shifts, dealt, at, xs, first),
        in_specs=SMEM_VMEM(2, 4 + len(sts) + len(qs)),
        out_shape=[
            jax.ShapeDtypeStruct((genes + (8 if last else 0), wide), F32),
            jax.ShapeDtypeStruct((16, wide), F32),
        ],
        name="grads",
    )(me, ent, ids, totals, slab, extra, *sts, *qs)


def gather_rows(n, unit, me_ref, offsets, blocks, hi, lo):
    own = unit // n
    for d, block in zip(offsets, blocks):
        p = lax.rem(me_ref[0] + d + n, n)
        for j in range(hi.shape[0] // unit):
            h, lw = split(block[j * own : (j + 1) * own, :])
            at = pl.ds(pl.multiple_of(j * unit + p * own, own), own)
            hi[at, :] = h
            lo[at, :] = lw


def product(exprs, hi, lo, lanes):
    eh, el = split(jnp.concatenate([e[...] for e in exprs], 1))
    gh, gl = hi[:, lanes], lo[:, lanes]
    return mm(eh, gh) + mm(eh, gl) + mm(el, gh)


def bwd_first_kernel(n, unit, offsets, priors, me_ref, *refs):
    out_ref, hi, lo = refs[-3:]
    prior, refs = refs[:priors], refs[priors:]
    blocks = refs[: len(offsets)]
    exprs = refs[len(offsets) : -3]

    @pl.when(pl.program_id(0) == 0)
    def _():
        gather_rows(n, unit, me_ref, offsets, blocks, hi, lo)

    total = product(exprs, hi, lo, slice(None))
    for p in prior:
        total = total + p[...]
    out_ref[...] = total


def bwd_last_kernel(n, unit, offsets, scale, splits, me_ref, *refs):
    x_ref, kept_ref, tot_ref, aux_ref = refs[:4]
    refs = refs[4:]
    priors, refs = refs[: len(splits)], refs[len(splits) :]
    grad_ref, filt_ref, hi, lo, back = refs[-5:]
    blocks = refs[: len(offsets)]
    exprs = refs[len(offsets) : -5]
    layers, rows, cols = x_ref.shape

    @pl.when(pl.program_id(0) == 0)
    def _():
        gather_rows(n, unit, me_ref, offsets, blocks, hi, lo)
        total = blocks[0][-8:, :]
        for b in blocks[1:]:
            total += b[-8:, :]
        back[...] = total
        for l in range(layers):
            lane = slice(l * cols, (l + 1) * cols)
            inv = 1.0 / tot_ref[-8:-7, lane]
            mass = tot_ref[-7:-6, lane] * inv
            back[2:3, lane] = inv
            back[3:4, lane] = total[0:1, lane] + aux_ref[1:2, lane] * mass

    for l in range(layers):
        lane = slice(l * cols, (l + 1) * cols)
        gw = product(exprs, hi, lo, lane)
        if splits:
            held = [p[:, lane] for p in priors]
            gw = gw + functools.reduce(
                lambda low, j: jnp.where(pl.program_id(0) < splits[j], low, held[j]),
                range(1, len(held)),
                held[0],
            )
        gw = gw + aux_ref[1:2, lane]
        mapping = jnp.exp(x_ref[l]) * back[2:3, lane]
        kept = jnp.transpose(jnp.broadcast_to(kept_ref[l], (128, rows)))
        kept = jnp.tile(kept, (1, cols // 128))
        grad_ref[l] = scale * (mapping * (kept * gw - back[3:4, lane]))
        share = mapping * gw
        lanes = share[:, 0:128]
        for c in range(128, cols, 128):
            lanes = lanes + share[:, c : c + 128]
        filt_ref[l] = jnp.sum(jnp.transpose(lanes), axis=0, keepdims=True)


def backward_first(n, unit, offsets, me, prior, blocks, exprs, begin, rows):
    tile = 256 if rows % 256 == 0 else rows
    wide = blocks[0].shape[1]
    genes = sum(w for _, _, w in exprs)
    skip = begin // tile
    whole = pl.BlockSpec(blocks[0].shape, lambda i: (0, 0))
    return pl.pallas_call(
        functools.partial(bwd_first_kernel, n, unit, offsets, len(prior)),
        grid=(rows // tile,),
        in_specs=[pl.BlockSpec(memory_space=pltpu.SMEM)]
        + [pl.BlockSpec((tile, wide), lambda i: (i, 0))] * len(prior)
        + [whole] * len(blocks)
        + [pl.BlockSpec((tile, w), lambda i, c=c: (i + skip, c)) for _, c, w in exprs],
        out_specs=pl.BlockSpec((tile, wide), lambda i: (i, 0)),
        out_shape=jax.ShapeDtypeStruct((rows, wide), F32),
        scratch_shapes=[pltpu.VMEM((genes, wide), BF16), pltpu.VMEM((genes, wide), BF16)],
        name="bwd_first",
        cost_estimate=COST,
    )(me, *prior, *blocks, *[e for e, _, _ in exprs])


def backward_last(n, unit, offsets, scale, me, x, kept, totals, aux, prior, blocks, exprs):
    tile = 256
    layers, rows, cols = x.shape
    wide = layers * cols
    genes = sum(w for _, _, w in exprs)
    fixed = lambda a: pl.BlockSpec(a.shape, lambda i: (0,) * a.ndim)
    args = [me, x, kept.reshape(layers, 1, rows), totals, aux]
    in_specs = [
        pl.BlockSpec(memory_space=pltpu.SMEM),
        pl.BlockSpec((layers, tile, cols), lambda i: (0, i, 0)),
        pl.BlockSpec((layers, 1, tile), lambda i: (0, 0, i)),
        fixed(totals),
        fixed(aux),
    ]
    args += prior
    splits = []
    for p in prior:
        begin = splits[-1] + prior[len(splits) - 1].shape[0] // tile if splits else 0
        splits.append(begin)
        steps = p.shape[0] // tile
        in_specs.append(
            pl.BlockSpec(
                (tile, wide), lambda i, b=begin, t=steps: (jnp.clip(i - b, 0, t - 1), 0)
            )
        )
    args += list(blocks) + [e for e, _, _ in exprs]
    in_specs += [fixed(b) for b in blocks]
    in_specs += [pl.BlockSpec((tile, w), lambda i, c=c: (i, c)) for _, c, w in exprs]
    return pl.pallas_call(
        functools.partial(bwd_last_kernel, n, unit, offsets, scale, splits),
        grid=(rows // tile,),
        in_specs=in_specs,
        out_specs=[
            pl.BlockSpec((layers, tile, cols), lambda i: (0, i, 0)),
            pl.BlockSpec((layers, 1, tile), lambda i: (0, 0, i)),
        ],
        out_shape=[
            jax.ShapeDtypeStruct((layers, rows, cols), F32),
            jax.ShapeDtypeStruct((layers, 1, rows), F32),
        ],
        scratch_shapes=[
            pltpu.VMEM((genes, wide), BF16),
            pltpu.VMEM((genes, wide), BF16),
            pltpu.VMEM((8, wide), F32),
        ],
        name="bwd_last",
        cost_estimate=COST,
    )(*args)


class Ring:
    def __init__(self, n):
        self.n = n
        order = ring_order(n)
        self.place = [order.index(i) for i in range(n)]
        right = [(order[i], order[(i + 1) % n]) for i in range(n)]
        self.dirs = (right, [(b, a) for a, b in right])
        self.far = n // 2
        self.near = n - 1 - self.far

    def hop(self, v, way):
        return lax.ppermute(v, "cell", self.dirs[way])


class Scatter:
    def __init__(self, ring, clock, v, flip):
        self.ring, self.clock, self.v, self.flip = ring, clock, v, flip
        self.sign = -1 if flip else 1
        self.step = 0
        self.r, self.l = self.at(ring.far), self.at(-ring.near)
        self.hop()

    def at(self, d):
        return self.v[(self.sign * d) % self.ring.n]

    def hop(self):
        self.r = self.ring.hop(self.r, int(self.flip))
        if self.step < self.ring.near:
            self.l = self.ring.hop(self.l, 1 - int(self.flip))
        self.step += 1

    def wait(self):
        self.r, self.l = self.clock.after(self.r, self.l)

    def advance(self):
        ring, s = self.ring, self.step - 1
        if s < ring.far - 1:
            self.r = self.r + self.at(ring.far - 1 - s)
        if s < ring.near - 1:
            self.l = self.l + self.at(s + 1 - ring.near)
        if self.step == ring.far:
            self.r = self.r + self.l + self.at(0)
        if self.step < ring.near:
            self.r, self.l = self.clock.after(self.r, self.l)
        else:
            (self.r,) = self.clock.after(self.r)
        if self.step < ring.far:
            self.hop()
            return True
        return False


class Gather:
    def __init__(self, ring, clock, v, flip):
        self.ring, self.clock, self.flip = ring, clock, flip
        self.sign = -1 if flip else 1
        self.blocks, self.offsets = [v], [0]
        self.r = self.l = v
        self.step = 0
        self.hop()

    def hop(self):
        self.step += 1
        self.r = self.ring.hop(self.r, int(self.flip))
        if self.step <= self.ring.near:
            self.l = self.ring.hop(self.l, 1 - int(self.flip))

    def wait(self):
        if self.step <= self.ring.near:
            self.r, self.l = self.clock.after(self.r, self.l)
        else:
            (self.r,) = self.clock.after(self.r)

    def advance(self):
        ring = self.ring
        self.blocks.append(self.r)
        self.offsets.append(-self.sign * self.step)
        if self.step <= ring.near:
            self.blocks.append(self.l)
            self.offsets.append(self.sign * self.step)
        if self.step < ring.far:
            self.hop()
            return True
        return False


def slot(*chains):
    for c in chains:
        c.wait()
    return any([c.advance() for c in chains])


def finish(chain):
    while slot(chain):
        pass


def on_device(logits, filter_logits, expression, observed, gene_mask, slide_ids, true_counts):
    layers, cell_rows, spot_cols = logits.shape
    n = lax.axis_size("cell")
    spots = lax.axis_size("spot")
    cells_all = cell_rows * n
    xs = spots // 2
    width = expression.shape[1]
    widths = SETS if sum(SETS) == width and all(w % (16 * n) == 0 for w in SETS) else [width]
    starts = [sum(widths[:h]) for h in range(len(widths))]
    owns = [w // n for w in widths]
    unit = math.gcd(*widths)
    sets = len(widths)
    ring = Ring(n)
    table = [
        [place] + [(q // 2 - dx) % xs * 2 + (q + dc) % 2 for dx in range(xs) for dc in range(2)]
        for place in ring.place
        for q in range(spots)
    ]
    me = lax.dynamic_index_in_dim(
        jnp.asarray(table, jnp.int32), lax.axis_index(("cell", "spot")), keepdims=False
    )

    def send(v, dx, dc):
        pairs = []
        for s in range(spots):
            x, c = s // 2, s % 2
            pairs.append((s, ((x + dx) % xs) * 2 + (c ^ dc)))
        return lax.ppermute(v, "spot", pairs)

    expr, far = {}, {}
    clock = Clock(me)

    def begin_x(h):
        (held,) = clock.after(expression)
        (piece,) = clock.after(held[:, starts[h] : starts[h] + widths[h]])
        for dx in range(1, xs):
            far[dx, h] = send(piece, dx, 0)

    begin_x(0)
    partner = send(clock.after(expression)[0], 0, 1)
    for h in range(sets):
        col = starts[h] // widths[h]
        expr[0, 0, h] = (expression, col, widths[h])
        expr[0, 1, h] = (partner, col, widths[h])

    kept = jax.nn.sigmoid(filter_logits)
    slab, units = deal(ring, unit, clock, observed, gene_mask)
    (kept,) = clock.after(kept)
    hi, lo, sums = prep(logits, kept)
    hi, lo, sums = clock.after(hi, lo, sums)
    away = range(1, xs)

    def project(chosen, dxs, flip, sums=None):
        parts = [
            (expr[dx, dc, h][0], expr[dx, dc, h][1] * widths[h], widths[h])
            for h in chosen
            for dx in dxs
            for dc in range(2)
        ]
        out = forward(n, unit, clock.token, hi, lo, parts, sums)
        out = clock.after(*out)
        return Scatter(ring, clock, out, flip)

    def begin_far(h):
        for dx in range(1, xs):
            (piece,) = clock.after(far[dx, h])
            expr[dx, 0, h] = (piece, 0, widths[h])
            expr[dx, 1, h] = (send(piece, 0, 1), 0, widths[h])

    ids = slide_ids.reshape(1, spot_cols)
    shifts = [(dx, dc) for dx in range(xs) for dc in range(2)]
    held = {
        "extra": jnp.broadcast_to(
            jnp.pad(true_counts.astype(F32), (0, 8 - SLIDES), constant_values=1.0)[:, None],
            (8, 2 * xs * owns[0]),
        )
    }

    def rows_of(h):
        at = Dealt(
            units, width // unit, starts[h] // unit, widths[h] // unit, unit // n, layers, 2 * xs
        )
        return at, [near[h].r, rings[h].r], [(0, 2 * owns[h]), (0, 2 * (xs - 1) * owns[h])]

    def take_stats(h):
        dealt, qs, at = rows_of(h)
        st = stats(dealt, clock.token, ids, near[0].r, slab, qs, at, h == 0)
        (st,) = clock.after(st)
        return [st] + [send(st, dx, dc) for dx, dc in shifts[1:]]

    def take_grads(h, sts):
        dealt, qs, at = rows_of(h)
        gp, more = grads(
            shifts,
            dealt,
            xs,
            clock.token,
            entropy,
            ids,
            near[0].r,
            slab,
            held["extra"],
            sts,
            qs,
            at,
            h == 0,
            h == sets - 1,
        )
        held["extra"] = more
        if h == 0:
            held["aux"] = more
        (gp,) = clock.after(gp)
        return Gather(ring, clock, gp, h % 2 == 0)

    if cell_rows % 256 == 0 and cell_rows >= 768:
        cuts = [256 * -(-i * (cell_rows // 256) // 3) for i in range(4)]
    else:
        cuts = [0, cell_rows]
    shares = [(begin, end - begin) for begin, end in zip(cuts, cuts[1:])]
    parts = len(shares)
    prior = [[] for _ in range(parts)]

    def multiply_back(h, j):
        prior[j] = [
            backward_first(
                n,
                unit,
                gathers[h].offsets,
                clock.token,
                prior[j],
                gathers[h].blocks,
                [expr[dx, dc, h] for dx in range(xs) for dc in range(2)],
                *shares[j],
            )
        ]
        prior[j] = clock.after(prior[j][0])

    rings, gathers = [], []
    near = [project([0], [0], False, sums)]
    (slab,) = clock.after(slab)
    scores, gates = clock.after(filter_logits, kept)
    entropy = jnp.sum(
        gates * jax.nn.softplus(-scores) + (1.0 - gates) * jax.nn.softplus(scores)
    ).reshape(1)
    for h in range(1, sets):
        near.append(project([h], [0], h % 2 == 1))
        begin_x(h)
    if sets == 2:
        slot(near[0])
        begin_far(0)
        rings.append(project([0], away, True))
        slot(near[0], near[1])
        slot(near[0], near[1], rings[0])
        slot(near[0], near[1], rings[0])
        begin_far(1)
        rings.append(project([1], away, False))
        slot(near[1], rings[0])
        slot(rings[0], rings[1])
        sts = take_stats(0)
        slot(rings[1])
        gathers.append(take_grads(0, sts))
        slot(rings[1], gathers[0])
        slot(rings[1], gathers[0])
        sts = take_stats(1)
        finish(gathers[0])
        gathers.append(take_grads(1, sts))
        for j in range(parts):
            multiply_back(0, j)
            slot(gathers[1])
        finish(gathers[1])
    else:
        for q in near:
            finish(q)
        for h in range(sets):
            begin_far(h)
            rings.append(project([h], away, True))
            finish(rings[h])
            gathers.append(take_grads(h, take_stats(h)))
            finish(gathers[h])
        for h in range(sets - 1):
            for j in range(parts):
                multiply_back(h, j)
    totals, aux = near[0].r, held["aux"]
    blocks, offsets = gathers[-1].blocks, gathers[-1].offsets
    exprs = [expr[dx, dc, sets - 1] for dx in range(xs) for dc in range(2)]
    grad_logits, filt = backward_last(
        n,
        unit,
        offsets,
        float(cells_all * G),
        clock.token,
        logits,
        kept,
        totals,
        aux,
        [p for ps in prior for p in ps],
        blocks,
        exprs,
    )
    tails = sum(b[-8:] for b in blocks)
    count_terms = jnp.stack([aux[8 : 8 + SLIDES, l * spot_cols] for l in range(layers)])
    loss = jnp.sum(tails[1]) + jnp.sum(count_terms) + ENTROPY_WEIGHT * tails[-1, 0] / cells_all
    filt = filt.reshape(layers, cell_rows)
    grad_kept = filt
    for dx, dc in shifts[1:]:
        grad_kept = grad_kept + send(filt, dx, dc)
    slope = kept * (1.0 - kept)
    grad_filter = cells_all * (grad_kept * slope - ENTROPY_WEIGHT * slope * filter_logits / cells_all)
    return (grad_logits, grad_filter, count_terms, loss)


def solution(mesh):
    in_specs = (
        P(None, "cell", "spot"),
        P(None, "cell"),
        P("cell", "spot"),
        P(None, "cell", "spot"),
        P(None, "cell"),
        P("spot"),
        P(),
    )
    out_specs = (P(None, "cell", "spot"), P(None, "cell"), P(), P())
    return jax.shard_map(
        on_device, mesh=mesh, in_specs=in_specs, out_specs=out_specs, check_vma=False
    )
```
